128 devices in a mesh: section: 8 (over z, core), expert: 16 (over y, x).
Axes of the slice: x: 4, y: 4, z: 4, core: 2. Of those that a mesh axis runs over, the one named last changes fastest.
Arguments:
- tokens_in: bfloat16 [2, 2048, 1024], P(None, 'expert'), may hold values from -6 to 6
- ln_gain: float32 [8, 1024], P('section'), may hold values from 0.1 to 1.9
- router: bfloat16 [8, 1024, 32], P('section'), may hold values from -0.1875 to 0.1875
- dense_in: bfloat16 [8, 1024, 2048], P('section'), may hold values from -0.1875 to 0.1875
- dense_out: bfloat16 [8, 2048, 1024], P('section'), may hold values from -0.125 to 0.125
- expert_in: bfloat16 [8, 32, 1024, 2048], P('section', 'expert'), may hold values from -0.1875 to 0.1875
- expert_out: bfloat16 [8, 32, 2048, 1024], P('section', 'expert'), may hold values from -0.125 to 0.125
- routes: int32 [8, 2, 2048, 1], P('section', None, 'expert'), may hold values from 0 to 31; in each aligned block of 64 rows (0 to 63, 64 to 127, ..., all dimensions but the last counted through in order) at most 4 rows name the same one
Outputs:
- tokens_out: bfloat16 [2, 2048, 1024], P(None, 'expert', 'section')
The draws below stay inside these ranges and needn't reach their ends.
Inputs may be any that keep to these rules, and one draw needn't show every extreme that they name: Split every row of 2048 tokens of routes into aligned blocks of 64 tokens. In no block does one id occur more than 4 times, and in every draw some id occurs exactly 4 times in some block.
All inputs are finite; a program needn't handle non-finite values.
Results may differ from the reference program's by a relative error of at most 0.019.
Values may be sent and summed in bfloat16 or wider, within the bound.
No kernel may reach another device: no remote copies, remote signals or barrier semaphores. Data moves between devices by JAX's collectives and lax.ppermute only.
A program may use at most 128 MiB of HBM per device.

```python
import math
import jax
import jax.numpy as jnp
import numpy as np
from jax import lax

D = 1024
FF = 2048
EXPERTS_LATE = 32
TOK_DEV = 128
M = 2
TOKENS = 2048
HCAP = 4
N_SECTION = 8
N_EXPERT = 16


def level_of(own_key, dims, shards, smallest, largest):
    factor_of = 1.0
    for dim, blocks in shards:
        steps = jax.random.uniform(jax.random.fold_in(jax.random.fold_in(own_key, 6), dim), (blocks,), jnp.float32, smallest / len(shards), largest / len(shards))
        factor_of = factor_of * jnp.repeat(jnp.exp(steps), dims[dim] // blocks).reshape((-1,) + (1,) * (len(dims) - 1 - dim))
    return factor_of


def shared_out(own_key, own, number, rows, number_of, top, bound, lean):
    ranking = jax.random.permutation(own_key, number_of)
    packed, usual = load_shares(number_of, rows * top, bound, lean, True), load_shares(number_of, rows * top, bound, lean, False)
    places = jnp.arange(number_of)

    def named(lengths, offset_by):
        used = int((lengths > 0).sum())
        fixed = max(1, used // 4)
        passed = fixed + (places - fixed + offset_by * (used - fixed)) % max(1, number_of - fixed)
        return jnp.zeros((number_of,), jnp.int32).at[ranking[jnp.where(places < fixed, places, passed)]].set(jnp.asarray(lengths, jnp.int32))

    lengths = jnp.where(number % 4 == 0, named(packed, number // 4), named(usual, number - number // 4 - 1))
    mixed = jax.random.permutation(jax.random.fold_in(own, 3), number_of)
    donor, receiver = mixed[0:number_of // 2 * 2:2], mixed[1:number_of // 2 * 2:2]
    margin = jnp.minimum(lengths[donor] - 1, bound - lengths[receiver]) // 2
    margin = jnp.where((donor == ranking[0]) | (receiver == ranking[0]) | (lengths[receiver] == 0), 0, jnp.maximum(margin, 0))
    passed = jax.random.randint(jax.random.fold_in(own, 4), (number_of // 2,), 0, 1 << 20) % (margin + 1)
    lengths = lengths.at[donor].add(-passed).at[receiver].add(passed)
    items = jnp.searchsorted(jnp.cumsum(lengths), jnp.arange(rows * top), side="right").astype(jnp.int32)
    listing = items.reshape(top, rows).T
    listing = listing[jax.random.permutation(jax.random.fold_in(own, 1), rows)]
    offset_by = jax.random.randint(jax.random.fold_in(own, 2), (rows, 1), 0, top)
    return jnp.take_along_axis(listing, (jnp.arange(top)[None, :] + offset_by) % top, axis=1)


def load_shares(amount, total, bound, slope, full):
    weights = [(1 << 20) // math.isqrt(grade ** slope) + 1 for grade in range(1, amount + 1)]
    largest = bound if full else min(bound, max(-(-total // amount), total * weights[0] // sum(weights)))
    least = 1 if total - largest >= amount - 1 else 0
    counts, surplus = [largest] + [least] * (amount - 1), total - largest - least * (amount - 1)
    while surplus > 0:
        movable = [i for i in range(1, amount) if counts[i] < largest] or [i for i in range(1, amount) if counts[i] < bound]
        pool, budget = sum([weights[i] for i in movable]), surplus
        for i in movable:
            more = min(bound - counts[i], max(1, budget * weights[i] // pool), surplus)
            counts[i] = counts[i] + more
            surplus = surplus - more
    return np.array(counts)


def normal_values(stream_key, extent, spread, bound, pieces=(), kind=jnp.bfloat16):
    values = spread * jax.random.normal(stream_key, extent, jnp.float32)
    if pieces:
        values = values * level_of(stream_key, extent, pieces, -0.22, 0.18)
    return jnp.clip(values, -bound, bound).astype(kind)


def setup_inputs(seed: int = 0) -> dict:
    seeds = jax.random.split(jax.random.key(seed), 9)
    tokens_in = normal_values(seeds[0], (M, TOKENS, D), 1.0, 6.0, ((1, 16),))
    ln_gain = jnp.clip(1.0 + 0.18 * jax.random.normal(seeds[1], (N_SECTION, D), jnp.float32), 0.1, 1.9)
    router = normal_values(seeds[2], (N_SECTION, D, EXPERTS_LATE), D ** -0.5, 0.1875, ((0, 8),))
    dense_in = normal_values(seeds[3], (N_SECTION, D, FF), D ** -0.5, 0.1875, ((0, 8),))
    dense_out = normal_values(seeds[4], (N_SECTION, FF, D), FF ** -0.5, 0.125, ((0, 8),))
    expert_in = normal_values(seeds[5], (N_SECTION, EXPERTS_LATE, D, FF), D ** -0.5, 0.1875, ((0, 8), (1, 16)))
    expert_out = normal_values(seeds[6], (N_SECTION, EXPERTS_LATE, FF, D), FF ** -0.5, 0.125, ((0, 8), (1, 16)))
    routes_keys = jax.random.split(jax.random.fold_in(seeds[7], 1), N_SECTION * M * TOKENS // (TOK_DEV // 2))
    routes_turns = jax.random.permutation(jax.random.fold_in(seeds[7], 3), N_SECTION * M * TOKENS // (TOK_DEV // 2))
    routes = jax.vmap(lambda own, number: shared_out(jax.random.fold_in(seeds[7], 2), own, number, TOK_DEV // 2, EXPERTS_LATE, 1, HCAP, 2))(routes_keys, routes_turns).reshape((N_SECTION, M, TOKENS, 1))
    return {"tokens_in": tokens_in, "ln_gain": ln_gain, "router": router, "dense_in": dense_in, "dense_out": dense_out, "expert_in": expert_in, "expert_out": expert_out, "routes": routes}


def norm_rows(stream, norm_gain):
    stream_float = stream.astype(jnp.float32)
    row_mean = lax.optimization_barrier(jnp.mean(stream_float, axis=-1, keepdims=True))
    centred = stream_float - row_mean
    row_var = lax.optimization_barrier(jnp.mean(centred * centred, axis=-1, keepdims=True))
    normed = (centred * lax.rsqrt(row_var + 1e-05) * norm_gain).astype(jnp.bfloat16)
    return (stream_float, normed)

def moe_layer(stream, norm_gain, router_cols, weight_din, weight_dout, weight_ein, weight_eout, expert_ids, late_section):
    stream_float, normed = norm_rows(stream, norm_gain)
    hidden = jax.nn.gelu(jnp.dot(normed, weight_din, preferred_element_type=jnp.float32), approximate=True).astype(jnp.bfloat16)
    dense_part = jnp.dot(hidden, weight_dout, preferred_element_type=jnp.float32)
    logits = jnp.dot(normed, router_cols, preferred_element_type=jnp.float32)
    experts = jnp.arange(EXPERTS_LATE, dtype=jnp.int32)
    picked = expert_ids[:, None] == experts[None, :]
    gate_value = jax.nn.sigmoid(lax.optimization_barrier(jnp.sum(jnp.where(picked, logits, 0.0), axis=1)))
    block_ones = picked.astype(jnp.int32).reshape(N_EXPERT, TOK_DEV, EXPERTS_LATE)
    before = jnp.cumsum(block_ones, axis=1) - block_ones
    position = lax.optimization_barrier(jnp.sum(before * block_ones, axis=2)).reshape(-1)
    source = jnp.arange(TOKENS, dtype=jnp.int32) // TOK_DEV
    capacity = 2 * HCAP
    slot_index = (expert_ids * (N_EXPERT * capacity) + source * capacity + position).astype(jnp.int32)
    buffer = jnp.zeros((EXPERTS_LATE * N_EXPERT * capacity, D), jnp.bfloat16).at[slot_index].set(normed)
    buffer = buffer.reshape(EXPERTS_LATE, N_EXPERT * capacity, D)

    def run_expert(expert_index):
        buffer_rows = buffer[expert_index]
        weight_row = jnp.where(late_section, expert_index, 2 * (expert_index // 2)).astype(jnp.int32)
        activation = jax.nn.gelu(jnp.dot(buffer_rows, weight_ein[weight_row], preferred_element_type=jnp.float32), approximate=True).astype(jnp.bfloat16)
        return jnp.dot(activation, weight_eout[weight_row], preferred_element_type=jnp.float32).astype(jnp.bfloat16)
    results = lax.map(run_expert, experts).reshape(-1, D)
    routed = results[slot_index].astype(jnp.float32)
    return (stream_float + dense_part + gate_value[:, None] * routed).astype(jnp.bfloat16)

def reference(tokens_in, ln_gain, router, dense_in, dense_out, expert_in, expert_out, routes):
    finished = []
    for micro_index in range(M):
        stream = tokens_in[micro_index]
        for section_number in range(N_SECTION):
            stream = moe_layer(stream, ln_gain[section_number], router[section_number], dense_in[section_number], dense_out[section_number], expert_in[section_number], expert_out[section_number], routes[section_number, micro_index, :, 0], section_number >= N_SECTION // 2)
        finished.append(stream)
    return jnp.stack(finished)
```

```python
import functools

import jax
import jax.numpy as jnp
from jax import lax
from jax.experimental import pallas as pl
from jax.experimental.pallas import tpu as pltpu
from jax.sharding import PartitionSpec as P

BF16 = jnp.bfloat16
F32 = jnp.float32
VMEM_SPEC = pl.BlockSpec(memory_space=pltpu.VMEM)
SMEM_SPEC = pl.BlockSpec(memory_space=pltpu.SMEM)
HBM_SPEC = pl.BlockSpec(memory_space=pl.ANY)
LIMIT = 30 << 20
PARTS = 4


def dot(a, b):
    return jnp.dot(a, b, preferred_element_type=F32)


def tables_kernel(ids_ref, send_ref, take_ref, picked_ref):
    blocks, tokens = ids_ref.shape
    slots = send_ref.shape[1]
    labels = picked_ref.shape[2]
    earlier = (
        lax.broadcasted_iota(jnp.int32, (tokens, tokens), 0)
        < lax.broadcasted_iota(jnp.int32, (tokens, tokens), 1)
    ).astype(BF16)
    capacity = slots // (labels // 4)
    for block in range(blocks):
        ids = ids_ref[block : block + 1, :]
        picked = (lax.broadcasted_iota(jnp.int32, (labels, tokens), 0) == ids).astype(F32)
        before = dot(picked.astype(BF16), earlier)
        position = jnp.sum(before * picked, axis=0, keepdims=True).astype(jnp.int32)
        slot = ids * capacity + position
        send = (lax.broadcasted_iota(jnp.int32, (slots, tokens), 0) == slot).astype(F32)
        send_ref[block] = send.astype(BF16)
        take_ref[block] = send.T.astype(BF16)
        picked_ref[block] = picked.T


def stream_of(info_ref, tokens_ref, received_ref):
    return jnp.where(info_ref[1] == 1, tokens_ref[info_ref[0]], received_ref[...])


def enter_kernel(info_ref, tokens_ref, received_ref, gain_ref, send_ref, normed_ref, outgoing_ref):
    stream = stream_of(info_ref, tokens_ref, received_ref).astype(F32)
    centred = stream - jnp.mean(stream, axis=-1, keepdims=True)
    variance = jnp.mean(centred * centred, axis=-1, keepdims=True)
    normed = (centred * lax.rsqrt(variance + 1e-05) * gain_ref[...]).astype(BF16)
    normed_ref[...] = normed
    outgoing_ref[...] = dot(send_ref[info_ref[0]], normed).astype(BF16)


def dense_kernel(
    parts,
    info_ref,
    tokens_ref,
    received_ref,
    normed_ref,
    picked_ref,
    router_ref,
    dense_in_ref,
    dense_out_ref,
    base_ref,
    gate_ref,
    in_ref,
    out_ref,
    sems,
):
    copies = fetches(dense_in_ref, dense_out_ref, in_ref, out_ref, sems, parts)
    for pair in copies:
        for copy in pair:
            copy.start()
    normed = normed_ref[...]
    logits = dot(normed, router_ref[...])
    labels = router_ref.shape[1]
    logit = jnp.sum(picked_ref[info_ref[0]][:, :labels] * logits, axis=1, keepdims=True)
    gate_ref[...] = jnp.broadcast_to(jax.nn.sigmoid(logit), gate_ref.shape)
    stream = stream_of(info_ref, tokens_ref, received_ref).astype(F32)
    base_ref[...] = stream + mlp(normed, in_ref, out_ref, copies)


def fetches(source_in, source_out, target_in, target_out, sems, parts):
    width = source_in.shape[1] // parts
    copies = []
    for part in range(parts):
        window = pl.ds(part * width, width)
        copies.append(
            (
                pltpu.make_async_copy(
                    source_in.at[:, window], target_in.at[:, window], sems.at[0, part]
                ),
                pltpu.make_async_copy(
                    source_out.at[window, :], target_out.at[window, :], sems.at[1, part]
                ),
            )
        )
    return copies


def mlp(token_rows, in_ref, out_ref, copies):
    width = in_ref.shape[1] // len(copies)
    total = None
    for part, (copy_in, copy_out) in enumerate(copies):
        window = pl.ds(part * width, width)
        copy_in.wait()
        activation = jax.nn.gelu(dot(token_rows, in_ref[:, window]), approximate=True).astype(BF16)
        copy_out.wait()
        product = dot(activation, out_ref[window, :])
        total = product if total is None else total + product
    return total


def expert_kernel(
    parts, info_ref, incoming_ref, expert_in_ref, expert_out_ref, result_ref, in_ref, out_ref, sems
):
    sources, rows, model_width = incoming_ref.shape
    half = rows // 2
    copies = [
        fetches(
            expert_in_ref.at[which],
            expert_out_ref.at[which],
            in_ref.at[which],
            out_ref.at[which],
            sems.at[which],
            parts,
        )
        for which in range(2)
    ]
    for pair in copies[0]:
        for copy in pair:
            copy.start()

    @pl.when(info_ref[2] == 1)
    def _():
        for pair in copies[1]:
            for copy in pair:
                copy.start()
        for which in range(2):
            window = pl.ds(which * half, half)
            token_rows = incoming_ref[:, window, :].reshape(sources * half, model_width)
            found = mlp(token_rows, in_ref.at[which], out_ref.at[which], copies[which])
            result_ref[:, window, :] = found.astype(BF16).reshape(sources, half, model_width)

    @pl.when(info_ref[2] == 0)
    def _():
        token_rows = incoming_ref[...].reshape(sources * rows, model_width)
        found = mlp(token_rows, in_ref.at[0], out_ref.at[0], copies[0])
        result_ref[...] = found.astype(BF16).reshape(sources, rows, model_width)


def leave_kernel(info_ref, base_ref, gate_ref, take_ref, returned_ref, stream_ref):
    routed = dot(take_ref[info_ref[0]], returned_ref[...])
    gate = gate_ref[:, :1]
    stream_ref[...] = (base_ref[...] + gate * routed).astype(BF16)


def split_kernel(first_ref, second_ref, out_ref):
    shares, tokens, share = out_ref.shape
    half = tokens // 2
    for number in range(shares):
        window = pl.ds(number * share, share)
        out_ref[number, :half, :] = first_ref[:, window]
        out_ref[number, half:, :] = second_ref[:, window]


def shape(dims, dtype):
    return jax.ShapeDtypeStruct(dims, dtype)


def body(tokens_in, ln_gain, router, dense_in, dense_out, expert_in, expert_out, routes):
    sections = lax.axis_size("section")
    members = lax.axis_size("expert")
    section_index = lax.axis_index("section")
    blocks, tok_dev, model_width = tokens_in.shape
    labels = router.shape[2]
    hidden_width = dense_in.shape[2]
    late = (section_index >= sections // 2).astype(jnp.int32)
    first = (section_index == 0).astype(jnp.int32)
    capacity = 2 * (tok_dev // labels)
    slots = labels * capacity
    params = pltpu.CompilerParams(vmem_limit_bytes=LIMIT)

    send, take, picked = pl.pallas_call(
        tables_kernel,
        out_shape=(
            shape((blocks, slots, tok_dev), BF16),
            shape((blocks, tok_dev, slots), BF16),
            shape((blocks, tok_dev, 128), F32),
        ),
        in_specs=[VMEM_SPEC],
        out_specs=[VMEM_SPEC] * 3,
        compiler_params=params,
    )(routes.reshape(blocks, tok_dev))

    def run(info, received):
        normed, outgoing = pl.pallas_call(
            enter_kernel,
            out_shape=(shape((tok_dev, model_width), BF16), shape((slots, model_width), BF16)),
            in_specs=[SMEM_SPEC] + [VMEM_SPEC] * 4,
            out_specs=[VMEM_SPEC] * 2,
            compiler_params=params,
        )(info, tokens_in, received, ln_gain, send)
        incoming = lax.all_to_all(
            outgoing.reshape(members, slots // members, model_width),
            "expert",
            split_axis=0,
            concat_axis=0,
            tiled=True,
        )
        base, gate = pl.pallas_call(
            functools.partial(dense_kernel, PARTS),
            out_shape=(shape((tok_dev, model_width), F32), shape((tok_dev, 128), F32)),
            in_specs=[SMEM_SPEC] + [VMEM_SPEC] * 5 + [HBM_SPEC] * 2,
            out_specs=[VMEM_SPEC] * 2,
            scratch_shapes=[
                pltpu.VMEM(dense_in.shape[1:], BF16),
                pltpu.VMEM(dense_out.shape[1:], BF16),
                pltpu.SemaphoreType.DMA((2, PARTS)),
            ],
            cost_estimate=pl.CostEstimate(
                flops=4 * tok_dev * model_width * hidden_width,
                transcendentals=tok_dev * hidden_width,
                bytes_accessed=8 << 20,
            ),
            compiler_params=params,
        )(info, tokens_in, received, normed, picked, router[0], dense_in[0], dense_out[0])
        results = pl.pallas_call(
            functools.partial(expert_kernel, PARTS),
            out_shape=shape(incoming.shape, BF16),
            in_specs=[SMEM_SPEC, VMEM_SPEC] + [HBM_SPEC] * 2,
            out_specs=VMEM_SPEC,
            scratch_shapes=[
                pltpu.VMEM(expert_in.shape[1:], BF16),
                pltpu.VMEM(expert_out.shape[1:], BF16),
                pltpu.SemaphoreType.DMA((2, 2, PARTS)),
            ],
            cost_estimate=pl.CostEstimate(
                flops=8 * tok_dev * model_width * hidden_width,
                transcendentals=2 * tok_dev * hidden_width,
                bytes_accessed=16 << 20,
            ),
            compiler_params=params,
        )(info, incoming, expert_in[0], expert_out[0])
        returned = lax.all_to_all(results, "expert", split_axis=0, concat_axis=0, tiled=True)
        return pl.pallas_call(
            leave_kernel,
            out_shape=shape((tok_dev, model_width), BF16),
            in_specs=[SMEM_SPEC] + [VMEM_SPEC] * 4,
            out_specs=VMEM_SPEC,
            compiler_params=params,
        )(info, base, gate, take, returned.reshape(slots, model_width))

    def step(number, carried):
        received, _, latest = carried
        block = number - section_index
        active = (block >= 0) & (block < blocks)
        info = jnp.stack([jnp.clip(block, 0, blocks - 1), first, late]).astype(jnp.int32)
        fresh = lax.cond(active, run, lambda info, received: received, info, received)
        received = lax.ppermute(
            fresh, "section", [(source, source + 1) for source in range(sections - 1)]
        )
        return received, latest, fresh

    nothing = jnp.zeros((tok_dev, model_width), BF16)
    _, before_last, last = lax.fori_loop(
        0, sections + blocks - 1, step, (nothing, nothing, nothing)
    )
    share = model_width // sections
    pieces = pl.pallas_call(
        split_kernel,
        out_shape=shape((sections, blocks * tok_dev, share), BF16),
        in_specs=[VMEM_SPEC] * 2,
        out_specs=VMEM_SPEC,
        compiler_params=params,
    )(before_last, last)
    spread = lax.all_to_all(pieces, "section", split_axis=0, concat_axis=0, tiled=True)
    return spread[sections - 1].reshape(blocks, tok_dev, share)


def solution(mesh):
    placed = (
        P(None, "expert", None),
        P("section", None),
        P("section", None, None),
        P("section", None, None),
        P("section", None, None),
        P("section", "expert", None, None),
        P("section", "expert", None, None),
        P("section", None, "expert", None),
    )
    return jax.shard_map(
        body, mesh=mesh, in_specs=placed, out_specs=P(None, "expert", "section"), check_vma=False
    )
```

```python
import functools

import jax
import jax.numpy as jnp
from jax import lax
from jax.experimental import pallas as pl
from jax.experimental.pallas import tpu as pltpu
from jax.sharding import PartitionSpec as P

BF16 = jnp.bfloat16
F32 = jnp.float32
VMEM_SPEC = pl.BlockSpec(memory_space=pltpu.VMEM)
SMEM_SPEC = pl.BlockSpec(memory_space=pltpu.SMEM)
HBM_SPEC = pl.BlockSpec(memory_space=pl.ANY)
LIMIT = 30 << 20
PARTS = 4


def dot(a, b):
    return jnp.dot(a, b, preferred_element_type=F32)


def tables_kernel(ids_ref, send_ref, take_ref, picked_ref):
    blocks, tokens = ids_ref.shape
    slots = send_ref.shape[1]
    labels = picked_ref.shape[2]
    earlier = (
        lax.broadcasted_iota(jnp.int32, (tokens, tokens), 0)
        < lax.broadcasted_iota(jnp.int32, (tokens, tokens), 1)
    ).astype(BF16)
    capacity = slots // (labels // 4)
    for block in range(blocks):
        ids = ids_ref[block : block + 1, :]
        picked = (lax.broadcasted_iota(jnp.int32, (labels, tokens), 0) == ids).astype(F32)
        before = dot(picked.astype(BF16), earlier)
        position = jnp.sum(before * picked, axis=0, keepdims=True).astype(jnp.int32)
        slot = ids * capacity + position
        send = (lax.broadcasted_iota(jnp.int32, (slots, tokens), 0) == slot).astype(F32)
        send_ref[block] = send.astype(BF16)
        take_ref[block] = send.T.astype(BF16)
        picked_ref[block] = picked.T


def enter_kernel(info_ref, received_ref, gain_ref, send_ref, normed_ref, outgoing_ref):
    stream = received_ref[...].astype(F32)
    centred = stream - jnp.mean(stream, axis=-1, keepdims=True)
    variance = jnp.mean(centred * centred, axis=-1, keepdims=True)
    normed = (centred * lax.rsqrt(variance + 1e-05) * gain_ref[...]).astype(BF16)
    normed_ref[...] = normed
    outgoing_ref[...] = dot(send_ref[info_ref[0]], normed).astype(BF16)


def dense_kernel(
    parts,
    info_ref,
    received_ref,
    normed_ref,
    picked_ref,
    router_ref,
    dense_in_ref,
    dense_out_ref,
    base_ref,
    gate_ref,
    in_ref,
    out_ref,
    sems,
):
    width = in_ref.shape[1] // parts
    copies = []
    for part in range(parts):
        window = pl.ds(part * width, width)
        copies.append(
            (
                pltpu.make_async_copy(
                    dense_in_ref.at[:, window], in_ref.at[:, window], sems.at[0, part]
                ),
                pltpu.make_async_copy(
                    dense_out_ref.at[window, :], out_ref.at[window, :], sems.at[1, part]
                ),
            )
        )
    for pair in copies:
        for copy in pair:
            copy.start()
    normed = normed_ref[...]
    logits = dot(normed, router_ref[...])
    labels = router_ref.shape[1]
    logit = jnp.sum(picked_ref[info_ref[0]][:, :labels] * logits, axis=1, keepdims=True)
    gate_ref[...] = jnp.broadcast_to(jax.nn.sigmoid(logit), gate_ref.shape)
    total = received_ref[...].astype(F32)
    dense_part = None
    for part, (copy_in, copy_out) in enumerate(copies):
        window = pl.ds(part * width, width)
        copy_in.wait()
        hidden = jax.nn.gelu(dot(normed, in_ref[:, window]), approximate=True).astype(BF16)
        copy_out.wait()
        product = dot(hidden, out_ref[window, :])
        dense_part = product if dense_part is None else dense_part + product
    base_ref[...] = total + dense_part


def mlp(token_rows, weight_in, weight_out):
    activation = jax.nn.gelu(dot(token_rows, weight_in), approximate=True).astype(BF16)
    return dot(activation, weight_out).astype(BF16)


def expert_kernel(info_ref, incoming_ref, expert_in_ref, expert_out_ref, result_ref):
    sources, rows, model_width = incoming_ref.shape
    half = rows // 2

    @pl.when(info_ref[1] == 1)
    def _():
        for which in range(2):
            window = pl.ds(which * half, half)
            token_rows = incoming_ref[:, window, :].reshape(sources * half, model_width)
            found = mlp(token_rows, expert_in_ref[which], expert_out_ref[which])
            result_ref[:, window, :] = found.reshape(sources, half, model_width)

    @pl.when(info_ref[1] == 0)
    def _():
        token_rows = incoming_ref[...].reshape(sources * rows, model_width)
        found = mlp(token_rows, expert_in_ref[0], expert_out_ref[0])
        result_ref[...] = found.reshape(sources, rows, model_width)


def leave_kernel(info_ref, base_ref, gate_ref, take_ref, returned_ref, stream_ref):
    routed = dot(take_ref[info_ref[0]], returned_ref[...])
    gate = gate_ref[:, :1]
    stream_ref[...] = (base_ref[...] + gate * routed).astype(BF16)


def split_kernel(first_ref, second_ref, out_ref):
    shares, tokens, share = out_ref.shape
    half = tokens // 2
    for number in range(shares):
        window = pl.ds(number * share, share)
        out_ref[number, :half, :] = first_ref[:, window]
        out_ref[number, half:, :] = second_ref[:, window]


def shape(dims, dtype):
    return jax.ShapeDtypeStruct(dims, dtype)


def body(tokens_in, ln_gain, router, dense_in, dense_out, expert_in, expert_out, routes):
    sections = lax.axis_size("section")
    members = lax.axis_size("expert")
    section_index = lax.axis_index("section")
    blocks, tok_dev, model_width = tokens_in.shape
    labels = router.shape[2]
    hidden_width = dense_in.shape[2]
    late = (section_index >= sections // 2).astype(jnp.int32)
    capacity = 2 * (tok_dev // labels)
    slots = labels * capacity
    params = pltpu.CompilerParams(vmem_limit_bytes=LIMIT)

    send, take, picked = pl.pallas_call(
        tables_kernel,
        out_shape=(
            shape((blocks, slots, tok_dev), BF16),
            shape((blocks, tok_dev, slots), BF16),
            shape((blocks, tok_dev, 128), F32),
        ),
        in_specs=[VMEM_SPEC],
        out_specs=[VMEM_SPEC] * 3,
        compiler_params=params,
    )(routes.reshape(blocks, tok_dev))

    def run(info, received):
        normed, outgoing = pl.pallas_call(
            enter_kernel,
            out_shape=(shape((tok_dev, model_width), BF16), shape((slots, model_width), BF16)),
            in_specs=[SMEM_SPEC] + [VMEM_SPEC] * 3,
            out_specs=[VMEM_SPEC] * 2,
            cost_estimate=pl.CostEstimate(
                flops=20_000_000_000, transcendentals=0, bytes_accessed=40 << 20
            ),
            compiler_params=params,
        )(info, received, ln_gain, send)
        incoming = lax.all_to_all(
            outgoing.reshape(members, slots // members, model_width),
            "expert",
            split_axis=0,
            concat_axis=0,
            tiled=True,
        )
        base, gate = pl.pallas_call(
            functools.partial(dense_kernel, PARTS),
            out_shape=(shape((tok_dev, model_width), F32), shape((tok_dev, 128), F32)),
            in_specs=[SMEM_SPEC] + [VMEM_SPEC] * 4 + [HBM_SPEC] * 2,
            out_specs=[VMEM_SPEC] * 2,
            scratch_shapes=[
                pltpu.VMEM(dense_in.shape[1:], BF16),
                pltpu.VMEM(dense_out.shape[1:], BF16),
                pltpu.SemaphoreType.DMA((2, PARTS)),
            ],
            cost_estimate=pl.CostEstimate(
                flops=4 * tok_dev * model_width * hidden_width,
                transcendentals=tok_dev * hidden_width,
                bytes_accessed=8 << 20,
            ),
            compiler_params=params,
        )(info, received, normed, picked, router[0], dense_in[0], dense_out[0])
        results = pl.pallas_call(
            expert_kernel,
            out_shape=shape(incoming.shape, BF16),
            in_specs=[SMEM_SPEC] + [VMEM_SPEC] * 3,
            out_specs=VMEM_SPEC,
            cost_estimate=pl.CostEstimate(
                flops=8 * tok_dev * model_width * hidden_width,
                transcendentals=2 * tok_dev * hidden_width,
                bytes_accessed=16 << 20,
            ),
            compiler_params=params,
        )(info, incoming, expert_in[0], expert_out[0])
        returned = lax.all_to_all(results, "expert", split_axis=0, concat_axis=0, tiled=True)
        return pl.pallas_call(
            leave_kernel,
            out_shape=shape((tok_dev, model_width), BF16),
            in_specs=[SMEM_SPEC] + [VMEM_SPEC] * 4,
            out_specs=VMEM_SPEC,
            compiler_params=params,
        )(info, base, gate, take, returned.reshape(slots, model_width))

    def step(number, carried):
        received, _, latest = carried
        block = number - section_index
        active = (block >= 0) & (block < blocks)
        info = jnp.stack([jnp.clip(block, 0, blocks - 1), late]).astype(jnp.int32)
        fresh = lax.cond(active, run, lambda info, received: tokens_in[blocks - 1], info, received)
        received = lax.ppermute(
            fresh, "section", [(source, (source + 1) % sections) for source in range(sections)]
        )
        return received, latest, fresh

    _, before_last, last = lax.fori_loop(
        0, sections + blocks - 1, step, (tokens_in[0], tokens_in[0], tokens_in[0])
    )
    share = model_width // sections
    pieces = pl.pallas_call(
        split_kernel,
        out_shape=shape((sections, blocks * tok_dev, share), BF16),
        in_specs=[VMEM_SPEC] * 2,
        out_specs=VMEM_SPEC,
        compiler_params=params,
    )(before_last, last)
    spread = lax.all_to_all(pieces, "section", split_axis=0, concat_axis=0, tiled=True)
    return spread[sections - 1].reshape(blocks, tok_dev, share)


def solution(mesh):
    placed = (
        P(None, "expert", None),
        P("section", None),
        P("section", None, None),
        P("section", None, None),
        P("section", None, None),
        P("section", "expert", None, None),
        P("section", "expert", None, None),
        P("section", None, "expert", None),
    )
    return jax.shard_map(
        body, mesh=mesh, in_specs=placed, out_specs=P(None, "expert", "section"), check_vma=False
    )
```

```python
import functools

import jax
import jax.numpy as jnp
from jax import lax
from jax.experimental import pallas as pl
from jax.experimental.pallas import tpu as pltpu
from jax.sharding import PartitionSpec as P

BF16 = jnp.bfloat16
F32 = jnp.float32
VMEM_SPEC = pl.BlockSpec(memory_space=pltpu.VMEM)
LIMIT = 30 << 20
TURNS = 8


def dot(a, b):
    return jnp.dot(a, b, preferred_element_type=F32)


def dot_t(a, b):
    return lax.dot_general(a, b, (((1,), (1,)), ((), ())), preferred_element_type=F32)


def tables_kernel(blocks, routes_ref, gain_ref, *refs):
    tokens_ref = refs[0] if len(refs) == 9 else None
    send_ref, take_ref, picked_ref, held_gain_ref = refs[1:5] if tokens_ref is not None else refs[:4]
    ids_ref, sems = refs[-2:]
    tokens = ids_ref.shape[1]
    moves = [(routes_ref, ids_ref), (gain_ref, held_gain_ref)]
    if tokens_ref is not None:
        moves += [(tokens_ref.at[0], refs[5]), (tokens_ref.at[1], refs[6])]
    copies = [
        pltpu.make_async_copy(source, target, sems.at[number])
        for number, (source, target) in enumerate(moves)
    ]
    for copy in copies:
        copy.start()
    copies[0].wait()
    slots = send_ref.shape[1]
    labels = picked_ref.shape[2]
    earlier = (
        lax.broadcasted_iota(jnp.int32, (tokens, tokens), 0)
        < lax.broadcasted_iota(jnp.int32, (tokens, tokens), 1)
    ).astype(BF16)
    capacity = slots // (labels // 4)
    for block in range(blocks):
        ids = ids_ref[block : block + 1, :]
        picked = (lax.broadcasted_iota(jnp.int32, (labels, tokens), 0) == ids).astype(F32)
        before = dot(picked.astype(BF16), earlier)
        position = jnp.sum(before * picked, axis=0, keepdims=True).astype(jnp.int32)
        slot = ids * capacity + position
        send = (lax.broadcasted_iota(jnp.int32, (slots, tokens), 0) == slot).astype(F32)
        send_ref[block] = send.astype(BF16)
        take_ref[block] = send.T.astype(BF16)
        picked_ref[block] = picked.T
    for copy in copies[1:]:
        copy.wait()


def of_block(pick_ref, table_ref):
    rows, lanes = table_ref.shape[1:]
    second = jnp.broadcast_to(pick_ref[:1, :1] == 1, (rows, lanes))
    return jnp.where(second, table_ref[1].astype(F32), table_ref[0].astype(F32))


def enter_kernel(pick_ref, received_ref, gain_ref, send_ref, normed_ref, outgoing_ref):
    stream = received_ref[...].astype(F32)
    centred = stream - jnp.mean(stream, axis=-1, keepdims=True)
    variance = jnp.mean(centred * centred, axis=-1, keepdims=True)
    normed = (centred * lax.rsqrt(variance + 1e-05) * gain_ref[...]).astype(BF16)
    normed_ref[...] = normed
    outgoing_ref[...] = dot(of_block(pick_ref, send_ref).astype(BF16), normed).astype(BF16)


def mlp(token_rows, weight_in, weight_out):
    activation = jax.nn.gelu(dot(token_rows, weight_in), approximate=True).astype(BF16)
    return dot(activation, weight_out)


def layer_kernel(
    pick_ref,
    received_ref,
    normed_ref,
    incoming_ref,
    picked_ref,
    router_ref,
    dense_in_ref,
    dense_out_ref,
    expert_in_ref,
    expert_out_ref,
    result_ref,
    base_ref,
    gate_ref,
):
    sources, rows, model_width = incoming_ref.shape
    half = rows // 2
    late = (lax.axis_index("section") >= lax.axis_size("section") // 2).astype(jnp.int32)
    normed = normed_ref[...]
    logits = dot_t(normed, router_ref[...])
    picked = of_block(pick_ref, picked_ref)[:, : logits.shape[1]]
    logit = jnp.sum(picked * logits, axis=1, keepdims=True)
    gate_ref[...] = jnp.broadcast_to(jax.nn.sigmoid(logit), gate_ref.shape)
    dense_part = mlp(normed, dense_in_ref[...], dense_out_ref[...])
    base_ref[...] = received_ref[...].astype(F32) + dense_part
    for which, held in ((0, 0), (1, late)):
        window = pl.ds(which * half, half)
        token_rows = incoming_ref[:, window, :].reshape(sources * half, model_width)
        found = mlp(token_rows, expert_in_ref[held], expert_out_ref[held]).astype(BF16)
        result_ref[:, window, :] = found.reshape(sources, half, model_width)


def stream_after(pick_ref, base_ref, gate_ref, take_ref, returned_ref):
    routed = dot(of_block(pick_ref, take_ref).astype(BF16), returned_ref[...])
    return (base_ref[...] + gate_ref[:, :1] * routed).astype(BF16)


def leave_kernel(pick_ref, base_ref, gate_ref, take_ref, returned_ref, stream_ref):
    stream_ref[...] = stream_after(pick_ref, base_ref, gate_ref, take_ref, returned_ref)


def put_shares(stream, out_ref):
    share = out_ref.shape[2]
    for number in range(out_ref.shape[0]):
        out_ref[number] = stream[:, number * share : (number + 1) * share]


def finish_kernel(pick_ref, base_ref, gate_ref, take_ref, returned_ref, out_ref):
    put_shares(stream_after(pick_ref, base_ref, gate_ref, take_ref, returned_ref), out_ref)


def split_kernel(stream_ref, out_ref):
    put_shares(stream_ref[...], out_ref)


def gather_kernel(pieces_ref, out_ref):
    out_ref[0] = pieces_ref[0]
    out_ref[1] = pieces_ref[pieces_ref.shape[0] - 1]


def untouched_kernel(*refs):
    pass


def wait_kernel(turns, source_ref, target_ref, sems):
    rows = source_ref.shape[0] // turns

    def turn(number, _):
        window = pl.ds(pl.multiple_of(number * rows, rows), rows)
        copy = pltpu.make_async_copy(source_ref.at[window], target_ref.at[window], sems.at[0])
        copy.start()
        copy.wait()
        return 0

    lax.fori_loop(0, turns, turn, 0)


def copy_over_kernel(*refs):
    count = len(refs) // 2
    sems = refs[-1]

    @pl.when(lax.axis_index("section") >= 2)
    def _():
        copies = [
            pltpu.make_async_copy(refs[n], refs[count + n], sems.at[n]) for n in range(count)
        ]
        for copy in copies:
            copy.start()
        for copy in copies:
            copy.wait()


def in_hbm(value):
    return pltpu.with_memory_space_constraint(value, pltpu.HBM)


def keep_kernel(source_ref, target_ref):
    target_ref[...] = source_ref[...]


def shape(dims, dtype):
    return jax.ShapeDtypeStruct(dims, dtype)


def kernel_call(kernel, inputs, outputs, cost=None):
    several = isinstance(outputs, tuple)
    return pl.pallas_call(
        kernel,
        out_shape=outputs,
        in_specs=[VMEM_SPEC] * inputs,
        out_specs=[VMEM_SPEC] * len(outputs) if several else VMEM_SPEC,
        cost_estimate=cost,
        compiler_params=pltpu.CompilerParams(vmem_limit_bytes=LIMIT),
    )


def body(tokens_in, ln_gain, router, dense_in, dense_out, expert_in, expert_out, routes):
    sections = lax.axis_size("section")
    members = lax.axis_size("expert")
    section_index = lax.axis_index("section")
    blocks, tok_dev, model_width = tokens_in.shape
    labels = router.shape[2]
    hidden_width = dense_in.shape[2]
    capacity = 2 * (tok_dev // labels)
    slots = labels * capacity
    share = model_width // sections
    stream_shape = shape((tok_dev, model_width), BF16)
    table_shapes = (
        shape((blocks, slots, tok_dev), BF16),
        shape((blocks, tok_dev, slots), BF16),
        shape((blocks, tok_dev, 128), F32),
        shape(ln_gain.shape, F32),
    )
    odd = section_index % 2
    own_block = odd

    def tables(ids, gain, *tokens):
        outputs = table_shapes + (stream_shape,) * (2 * len(tokens))
        return pl.pallas_call(
            functools.partial(tables_kernel, blocks),
            out_shape=outputs,
            in_specs=[pl.BlockSpec(memory_space=pltpu.HBM)] * (2 + len(tokens)),
            out_specs=[VMEM_SPEC] * len(outputs),
            scratch_shapes=[
                pltpu.VMEM((blocks, tok_dev), jnp.int32),
                pltpu.SemaphoreType.DMA((4,)),
            ],
            compiler_params=pltpu.CompilerParams(vmem_limit_bytes=LIMIT),
        )(*map(in_hbm, (ids, gain) + tokens))

    def pick(block):
        return jnp.full((8, 128), block, jnp.int32)

    def exchange(rows, axis):
        return lax.all_to_all(rows, axis, split_axis=0, concat_axis=0, tiled=True)

    ids = routes.reshape(blocks, tok_dev)
    router_rows = router[0].T
    weights = (dense_in[0], dense_out[0], expert_in[0], expert_out[0])
    *own_tables, first, second = tables(ids, ln_gain, tokens_in)
    own = (tuple(own_tables), router_rows, weights)

    def swapped():
        swap = [(source, source + 1 - 2 * (source % 2)) for source in range(sections)]
        arrays = weights + (router_rows, ids, ln_gain)
        *others, other_router, other_ids, other_gain = [
            lax.ppermute(value, "section", swap) for value in arrays
        ]
        return tuple(tables(other_ids, other_gain)), other_router, tuple(others)

    def nothing():
        outputs = table_shapes + (router_rows,) + weights
        found = pl.pallas_call(
            untouched_kernel,
            out_shape=tuple(shape(value.shape, value.dtype) for value in outputs),
            out_specs=[pl.BlockSpec(memory_space=pl.ANY)] * len(outputs),
        )()
        return tuple(found[:4]), found[4], tuple(found[5:])

    other = lax.cond(section_index >= 2, swapped, nothing)
    passed = pl.pallas_call(
        copy_over_kernel,
        out_shape=tuple(shape(value.shape, value.dtype) for value in other[2]),
        in_specs=[pl.BlockSpec(memory_space=pl.ANY)] * 4,
        out_specs=[pl.BlockSpec(memory_space=pl.ANY)] * 4,
        scratch_shapes=[pltpu.SemaphoreType.DMA((4,))],
    )(*other[2])
    other = (other[0], other[1], tuple(passed))

    def layer(block, received, context):
        (send, take, picked, gain), router_part, layer_weights = context
        chosen = pick(block)
        normed, outgoing = kernel_call(
            enter_kernel,
            4,
            (stream_shape, shape((slots, model_width), BF16)),
            pl.CostEstimate(flops=20_000_000_000, transcendentals=0, bytes_accessed=40 << 20),
        )(chosen, received, gain, send)
        incoming = exchange(outgoing.reshape(members, slots // members, model_width), "expert")
        results, base, gate = kernel_call(
            layer_kernel,
            10,
            (
                shape(incoming.shape, BF16),
                shape((tok_dev, model_width), F32),
                shape((tok_dev, 128), F32),
            ),
            pl.CostEstimate(
                flops=12 * tok_dev * model_width * hidden_width,
                transcendentals=3 * tok_dev * hidden_width,
                bytes_accessed=26 << 20,
            ),
        )(chosen, received, normed, incoming, picked, router_part, *layer_weights)
        returned = exchange(results, "expert").reshape(slots, model_width)
        return chosen, base, gate, take, returned

    def run(block, received, context):
        return kernel_call(leave_kernel, 5, stream_shape)(
            *layer(block, received, context)
        )

    def keep(stream):
        return kernel_call(keep_kernel, 1, stream_shape)(stream)

    def late_start(stream):
        return pl.pallas_call(
            functools.partial(wait_kernel, TURNS),
            out_shape=stream_shape,
            in_specs=[VMEM_SPEC],
            out_specs=VMEM_SPEC,
            scratch_shapes=[pltpu.SemaphoreType.DMA((1,))],
        )(stream)

    everyone = [(source, source) for source in range(sections)]
    pair = [(0, 1), (1, 0)] + everyone[2:]
    around = [(source, (source + 1) % sections) for source in range(sections)]
    odd_ring = everyone[0::2] + [(source, (source + 2) % sections) for source in range(1, sections, 2)]
    even_ring = everyone[1::2] + [(source, (source + 2) % sections) for source in range(0, sections, 2)]

    fresh = lax.cond(
        section_index == 0,
        lambda stream: run(0, stream, own),
        lambda stream: jnp.zeros((tok_dev, model_width), BF16),
        first,
    )
    arrived = lax.ppermute(fresh, "section", pair)
    waiting = lax.cond(
        section_index == 0,
        lambda stream: run(1, stream, own),
        lambda stream: jnp.zeros((tok_dev, model_width), BF16),
        second,
    )
    stream = lax.cond(
        section_index == 1,
        lambda arrived, waiting: run(0, late_start(arrived), own),
        lambda arrived, waiting: keep(waiting),
        arrived,
        waiting,
    )
    stream = lax.ppermute(stream, "section", around)

    def chip(number, stream):
        place = section_index - 2 * number
        stream = lax.cond(
            (place == -1) | (place == 0),
            lambda stream: run(own_block, stream, own),
            keep,
            stream,
        )
        stream = lax.cond(
            odd == 1, lambda stream: lax.ppermute(stream, "section", odd_ring), keep, stream
        )
        stream = lax.cond(
            (place == 0) | (place == 1),
            lambda stream: run(own_block, stream, other),
            keep,
            stream,
        )
        return lax.cond(
            odd == 0, lambda stream: lax.ppermute(stream, "section", even_ring), keep, stream
        )

    stream = lax.fori_loop(1, sections // 2, chip, stream)
    pieces_shape = shape((sections, tok_dev, share), BF16)
    pieces = lax.cond(
        section_index == sections - 1,
        lambda stream: kernel_call(finish_kernel, 5, pieces_shape)(*layer(1, stream, own)),
        lambda stream: kernel_call(split_kernel, 1, pieces_shape)(stream),
        stream,
    )
    return kernel_call(gather_kernel, 1, shape((blocks, tok_dev, share), BF16))(
        exchange(pieces, "section")
    )


def solution(mesh):
    placed = (
        P(None, "expert", None),
        P("section", None),
        P("section", None, None),
        P("section", None, None),
        P("section", None, None),
        P("section", "expert", None, None),
        P("section", "expert", None, None),
        P("section", None, "expert", None),
    )
    return jax.shard_map(
        body, mesh=mesh, in_specs=placed, out_specs=P(None, "expert", "section"), check_vma=False
    )
```

```python
import functools

import jax
import jax.numpy as jnp
from jax import lax
from jax.experimental import pallas as pl
from jax.experimental.pallas import tpu as pltpu
from jax.sharding import PartitionSpec as P

BF16 = jnp.bfloat16
F32 = jnp.float32
VMEM_SPEC = pl.BlockSpec(memory_space=pltpu.VMEM)
LIMIT = 30 << 20
TURNS = 8


def dot(a, b):
    return jnp.dot(a, b, preferred_element_type=F32)


def dot_t(a, b):
    return lax.dot_general(a, b, (((1,), (1,)), ((), ())), preferred_element_type=F32)


def make_tables(blocks, routes_ref, gain_ref, *refs):
    tokens_ref = refs[0] if len(refs) == 9 else None
    send_ref, take_ref, picked_ref, held_gain_ref = refs[1:5] if tokens_ref is not None else refs[:4]
    ids_ref, sems = refs[-2:]
    tokens = ids_ref.shape[1]
    moves = [(routes_ref, ids_ref), (gain_ref, held_gain_ref)]
    if tokens_ref is not None:
        moves += [(tokens_ref.at[0], refs[5]), (tokens_ref.at[1], refs[6])]
    copies = [
        pltpu.make_async_copy(source, target, sems.at[number])
        for number, (source, target) in enumerate(moves)
    ]
    for copy in copies:
        copy.start()
    copies[0].wait()
    slots = send_ref.shape[1]
    labels = picked_ref.shape[2]
    earlier = (
        lax.broadcasted_iota(jnp.int32, (tokens, tokens), 0)
        < lax.broadcasted_iota(jnp.int32, (tokens, tokens), 1)
    ).astype(BF16)
    capacity = slots // (labels // 4)
    for block in range(blocks):
        ids = ids_ref[block : block + 1, :]
        picked = (lax.broadcasted_iota(jnp.int32, (labels, tokens), 0) == ids).astype(F32)
        before = dot(picked.astype(BF16), earlier)
        position = jnp.sum(before * picked, axis=0, keepdims=True).astype(jnp.int32)
        slot = ids * capacity + position
        send = (lax.broadcasted_iota(jnp.int32, (slots, tokens), 0) == slot).astype(F32)
        send_ref[block] = send.astype(BF16)
        take_ref[block] = send.T.astype(BF16)
        picked_ref[block] = picked.T
    for copy in copies[1:]:
        copy.wait()


def tables_kernel(blocks, always, *refs):
    if always:
        make_tables(blocks, *refs)
    else:
        pl.when(lax.axis_index("section") >= 2)(functools.partial(make_tables, blocks, *refs))


def of_block(pick_ref, table_ref):
    rows, lanes = table_ref.shape[1:]
    second = jnp.broadcast_to(pick_ref[:1, :1] == 1, (rows, lanes))
    return jnp.where(second, table_ref[1].astype(F32), table_ref[0].astype(F32))


def enter_kernel(pick_ref, received_ref, gain_ref, send_ref, normed_ref, outgoing_ref):
    stream = received_ref[...].astype(F32)
    centred = stream - jnp.mean(stream, axis=-1, keepdims=True)
    variance = jnp.mean(centred * centred, axis=-1, keepdims=True)
    normed = (centred * lax.rsqrt(variance + 1e-05) * gain_ref[...]).astype(BF16)
    normed_ref[...] = normed
    outgoing_ref[...] = dot(of_block(pick_ref, send_ref).astype(BF16), normed).astype(BF16)


def mlp(token_rows, weight_in, weight_out):
    activation = jax.nn.gelu(dot(token_rows, weight_in), approximate=True).astype(BF16)
    return dot(activation, weight_out)


def layer_kernel(
    pick_ref,
    received_ref,
    normed_ref,
    incoming_ref,
    picked_ref,
    router_ref,
    dense_in_ref,
    dense_out_ref,
    expert_in_ref,
    expert_out_ref,
    result_ref,
    base_ref,
    gate_ref,
):
    sources, rows, model_width = incoming_ref.shape
    half = rows // 2
    late = (lax.axis_index("section") >= lax.axis_size("section") // 2).astype(jnp.int32)
    normed = normed_ref[...]
    logits = dot_t(normed, router_ref[...])
    picked = of_block(pick_ref, picked_ref)[:, : logits.shape[1]]
    logit = jnp.sum(picked * logits, axis=1, keepdims=True)
    gate_ref[...] = jnp.broadcast_to(jax.nn.sigmoid(logit), gate_ref.shape)
    dense_part = mlp(normed, dense_in_ref[...], dense_out_ref[...])
    base_ref[...] = received_ref[...].astype(F32) + dense_part
    for which, held in ((0, 0), (1, late)):
        window = pl.ds(which * half, half)
        token_rows = incoming_ref[:, window, :].reshape(sources * half, model_width)
        found = mlp(token_rows, expert_in_ref[held], expert_out_ref[held]).astype(BF16)
        result_ref[:, window, :] = found.reshape(sources, half, model_width)


def stream_after(pick_ref, base_ref, gate_ref, take_ref, returned_ref):
    routed = dot(of_block(pick_ref, take_ref).astype(BF16), returned_ref[...])
    return (base_ref[...] + gate_ref[:, :1] * routed).astype(BF16)


def leave_kernel(pick_ref, base_ref, gate_ref, take_ref, returned_ref, stream_ref):
    stream_ref[...] = stream_after(pick_ref, base_ref, gate_ref, take_ref, returned_ref)


def put_shares(stream, out_ref):
    share = out_ref.shape[2]
    for number in range(out_ref.shape[0]):
        out_ref[number] = stream[:, number * share : (number + 1) * share]


def finish_kernel(pick_ref, base_ref, gate_ref, take_ref, returned_ref, out_ref):
    put_shares(stream_after(pick_ref, base_ref, gate_ref, take_ref, returned_ref), out_ref)


def split_kernel(stream_ref, out_ref):
    put_shares(stream_ref[...], out_ref)


def gather_kernel(pieces_ref, out_ref):
    out_ref[0] = pieces_ref[0]
    out_ref[1] = pieces_ref[pieces_ref.shape[0] - 1]


def untouched_kernel(*refs):
    pass


def wait_kernel(turns, source_ref, target_ref, sems):
    rows = source_ref.shape[0] // turns

    def turn(number, _):
        window = pl.ds(pl.multiple_of(number * rows, rows), rows)
        copy = pltpu.make_async_copy(source_ref.at[window], target_ref.at[window], sems.at[0])
        copy.start()
        copy.wait()
        return 0

    lax.fori_loop(0, turns, turn, 0)


def copy_over_kernel(*refs):
    count = (len(refs) - 1) // 3
    sources, targets, stages, sems = refs[: count + 1], refs[count + 1 : 2 * count + 2], refs[2 * count + 2 : -1], refs[-1]

    @pl.when(lax.axis_index("section") >= 2)
    def _():
        reads = [
            pltpu.make_async_copy(source, stage, sems.at[0, n])
            for n, (source, stage) in enumerate(zip(sources, stages + targets[-1:]))
        ]
        writes = [
            pltpu.make_async_copy(stage, target, sems.at[1, n])
            for n, (stage, target) in enumerate(zip(stages, targets))
        ]
        for read in reads:
            read.start()
        for read, write in zip(reads, writes):
            read.wait()
            write.start()
        reads[-1].wait()
        for write in writes:
            write.wait()


def in_hbm(value):
    return pltpu.with_memory_space_constraint(value, pltpu.HBM)


def keep_kernel(source_ref, target_ref):
    target_ref[...] = source_ref[...]


def shape(dims, dtype):
    return jax.ShapeDtypeStruct(dims, dtype)


def kernel_call(kernel, inputs, outputs, cost=None):
    several = isinstance(outputs, tuple)
    return pl.pallas_call(
        kernel,
        out_shape=outputs,
        in_specs=[VMEM_SPEC] * inputs,
        out_specs=[VMEM_SPEC] * len(outputs) if several else VMEM_SPEC,
        cost_estimate=cost,
        compiler_params=pltpu.CompilerParams(vmem_limit_bytes=LIMIT),
    )


def body(tokens_in, ln_gain, router, dense_in, dense_out, expert_in, expert_out, routes):
    sections = lax.axis_size("section")
    members = lax.axis_size("expert")
    section_index = lax.axis_index("section")
    blocks, tok_dev, model_width = tokens_in.shape
    labels = router.shape[2]
    hidden_width = dense_in.shape[2]
    capacity = 2 * (tok_dev // labels)
    slots = labels * capacity
    share = model_width // sections
    stream_shape = shape((tok_dev, model_width), BF16)
    table_shapes = (
        shape((blocks, slots, tok_dev), BF16),
        shape((blocks, tok_dev, slots), BF16),
        shape((blocks, tok_dev, 128), F32),
        shape(ln_gain.shape, F32),
    )
    odd = section_index % 2
    own_block = odd

    def tables(always, ids, gain, *tokens):
        outputs = table_shapes + (stream_shape,) * (2 * len(tokens))
        return pl.pallas_call(
            functools.partial(tables_kernel, blocks, always),
            out_shape=outputs,
            in_specs=[pl.BlockSpec(memory_space=pltpu.HBM)] * (2 + len(tokens)),
            out_specs=[VMEM_SPEC] * len(outputs),
            scratch_shapes=[
                pltpu.VMEM((blocks, tok_dev), jnp.int32),
                pltpu.SemaphoreType.DMA((4,)),
            ],
            compiler_params=pltpu.CompilerParams(vmem_limit_bytes=LIMIT),
        )(*map(in_hbm, (ids, gain) + tokens))

    def pick(block):
        return jnp.full((8, 128), block, jnp.int32)

    def exchange(rows, axis):
        return lax.all_to_all(rows, axis, split_axis=0, concat_axis=0, tiled=True)

    ids = routes.reshape(blocks, tok_dev)
    router_rows = router[0].T
    weights = (dense_in[0], dense_out[0], expert_in[0], expert_out[0])
    *own_tables, first, second = tables(True, ids, ln_gain, tokens_in)
    own = (tuple(own_tables), router_rows, weights)

    def swapped():
        swap = [(source, source + 1 - 2 * (source % 2)) for source in range(sections)]
        arrays = weights + (router_rows, ids, ln_gain)
        return tuple(lax.ppermute(value, "section", swap) for value in arrays)

    def nothing():
        arrays = weights + (router_rows, ids, ln_gain)
        return tuple(
            pl.pallas_call(
                untouched_kernel,
                out_shape=tuple(shape(value.shape, value.dtype) for value in arrays),
                out_specs=[pl.BlockSpec(memory_space=pl.ANY)] * len(arrays),
            )()
        )

    *others, other_ids, other_gain = lax.cond(section_index >= 2, swapped, nothing)
    *other_weights, other_router = pl.pallas_call(
        copy_over_kernel,
        out_shape=tuple(shape(value.shape, value.dtype) for value in others),
        in_specs=[pl.BlockSpec(memory_space=pl.ANY)] * 5,
        out_specs=[pl.BlockSpec(memory_space=pl.ANY)] * 4 + [VMEM_SPEC],
        scratch_shapes=[pltpu.VMEM(value.shape, BF16) for value in weights]
        + [pltpu.SemaphoreType.DMA((2, 5))],
        compiler_params=pltpu.CompilerParams(vmem_limit_bytes=LIMIT),
    )(*others)
    other = (tuple(tables(False, other_ids, other_gain)), other_router, tuple(other_weights))

    def layer(block, received, context):
        (send, take, picked, gain), router_part, layer_weights = context
        chosen = pick(block)
        normed, outgoing = kernel_call(
            enter_kernel,
            4,
            (stream_shape, shape((slots, model_width), BF16)),
            pl.CostEstimate(flops=20_000_000_000, transcendentals=0, bytes_accessed=40 << 20),
        )(chosen, received, gain, send)
        incoming = exchange(outgoing.reshape(members, slots // members, model_width), "expert")
        results, base, gate = kernel_call(
            layer_kernel,
            10,
            (
                shape(incoming.shape, BF16),
                shape((tok_dev, model_width), F32),
                shape((tok_dev, 128), F32),
            ),
            pl.CostEstimate(
                flops=12 * tok_dev * model_width * hidden_width,
                transcendentals=3 * tok_dev * hidden_width,
                bytes_accessed=26 << 20,
            ),
        )(chosen, received, normed, incoming, picked, router_part, *layer_weights)
        returned = exchange(results, "expert").reshape(slots, model_width)
        return chosen, base, gate, take, returned

    def run(block, received, context):
        return kernel_call(leave_kernel, 5, stream_shape)(
            *layer(block, received, context)
        )

    def keep(stream):
        return kernel_call(keep_kernel, 1, stream_shape)(stream)

    def late_start(stream):
        return pl.pallas_call(
            functools.partial(wait_kernel, TURNS),
            out_shape=stream_shape,
            in_specs=[VMEM_SPEC],
            out_specs=VMEM_SPEC,
            scratch_shapes=[pltpu.SemaphoreType.DMA((1,))],
        )(stream)

    everyone = [(source, source) for source in range(sections)]
    pair = [(0, 1), (1, 0)] + everyone[2:]
    around = [(source, (source + 1) % sections) for source in range(sections)]
    odd_ring = everyone[0::2] + [(source, (source + 2) % sections) for source in range(1, sections, 2)]
    even_ring = everyone[1::2] + [(source, (source + 2) % sections) for source in range(0, sections, 2)]

    fresh = lax.cond(
        section_index == 0,
        lambda stream: run(0, stream, own),
        lambda stream: jnp.zeros((tok_dev, model_width), BF16),
        first,
    )
    arrived = lax.ppermute(fresh, "section", pair)
    waiting = lax.cond(
        section_index == 0,
        lambda stream: run(1, stream, own),
        lambda stream: jnp.zeros((tok_dev, model_width), BF16),
        second,
    )
    stream = lax.cond(
        section_index == 1,
        lambda arrived, waiting: run(0, late_start(arrived), own),
        lambda arrived, waiting: keep(waiting),
        arrived,
        waiting,
    )
    stream = lax.ppermute(stream, "section", around)

    def chip(number, stream):
        place = section_index - 2 * number
        stream = lax.cond(
            (place == -1) | (place == 0),
            lambda stream: run(own_block, stream, own),
            keep,
            stream,
        )
        stream = lax.cond(
            odd == 1, lambda stream: keep(lax.ppermute(stream, "section", odd_ring)), keep, stream
        )
        stream = lax.cond(
            (place == 0) | (place == 1),
            lambda stream: run(own_block, stream, other),
            keep,
            stream,
        )
        return lax.cond(
            odd == 0, lambda stream: keep(lax.ppermute(stream, "section", even_ring)), keep, stream
        )

    stream = lax.fori_loop(1, sections // 2, chip, stream)
    pieces_shape = shape((sections, tok_dev, share), BF16)
    pieces = lax.cond(
        section_index == sections - 1,
        lambda stream: kernel_call(finish_kernel, 5, pieces_shape)(*layer(1, stream, own)),
        lambda stream: kernel_call(split_kernel, 1, pieces_shape)(stream),
        stream,
    )
    return kernel_call(gather_kernel, 1, shape((blocks, tok_dev, share), BF16))(
        exchange(pieces, "section")
    )


def solution(mesh):
    placed = (
        P(None, "expert", None),
        P("section", None),
        P("section", None, None),
        P("section", None, None),
        P("section", None, None),
        P("section", "expert", None, None),
        P("section", "expert", None, None),
        P("section", None, "expert", None),
    )
    return jax.shard_map(
        body, mesh=mesh, in_specs=placed, out_specs=P(None, "expert", "section"), check_vma=False
    )
```

```python
import functools

import jax
import jax.numpy as jnp
from jax import lax
from jax.experimental import pallas as pl
from jax.experimental.pallas import tpu as pltpu
from jax.sharding import PartitionSpec as P

BF16 = jnp.bfloat16
F32 = jnp.float32
VMEM_SPEC = pl.BlockSpec(memory_space=pltpu.VMEM)
LIMIT = 30 << 20
TURNS = 36


def dot(a, b):
    return jnp.dot(a, b, preferred_element_type=F32)


def dot_t(a, b):
    return lax.dot_general(a, b, (((1,), (1,)), ((), ())), preferred_element_type=F32)


def make_tables(blocks, routes_ref, gain_ref, *refs):
    tokens_ref = refs[0] if len(refs) == 8 else None
    send_ref, picked_ref, held_gain_ref = refs[1:4] if tokens_ref is not None else refs[:3]
    ids_ref, sems = refs[-2:]
    tokens = ids_ref.shape[1]
    moves = [(routes_ref, ids_ref), (gain_ref, held_gain_ref)]
    if tokens_ref is not None:
        moves += [(tokens_ref.at[0], refs[4]), (tokens_ref.at[1], refs[5])]
    copies = [
        pltpu.make_async_copy(source, target, sems.at[number])
        for number, (source, target) in enumerate(moves)
    ]
    for copy in copies:
        copy.start()
    copies[0].wait()
    slots = send_ref.shape[1]
    labels = picked_ref.shape[2]
    earlier = (
        lax.broadcasted_iota(jnp.int32, (tokens, tokens), 0)
        < lax.broadcasted_iota(jnp.int32, (tokens, tokens), 1)
    ).astype(BF16)
    capacity = slots // (labels // 4)
    for block in range(blocks):
        ids = ids_ref[block : block + 1, :]
        picked = (lax.broadcasted_iota(jnp.int32, (labels, tokens), 0) == ids).astype(F32)
        before = dot(picked.astype(BF16), earlier)
        position = jnp.sum(before * picked, axis=0, keepdims=True).astype(jnp.int32)
        slot = ids * capacity + position
        send = (lax.broadcasted_iota(jnp.int32, (slots, tokens), 0) == slot).astype(F32)
        send_ref[block] = send.astype(BF16)
        picked_ref[block] = picked.T
    for copy in copies[1:]:
        copy.wait()


def tables_kernel(blocks, always, *refs):
    if always:
        make_tables(blocks, *refs)
    else:
        pl.when(lax.axis_index("section") >= 2)(functools.partial(make_tables, blocks, *refs))


def of_block(pick_ref, table_ref):
    rows, lanes = table_ref.shape[1:]
    second = jnp.broadcast_to(pick_ref[:1, :1] == 1, (rows, lanes))
    return jnp.where(second, table_ref[1].astype(F32), table_ref[0].astype(F32))


def enter_kernel(pick_ref, received_ref, gain_ref, send_ref, normed_ref, outgoing_ref):
    stream = received_ref[...].astype(F32)
    centred = stream - jnp.mean(stream, axis=-1, keepdims=True)
    variance = jnp.mean(centred * centred, axis=-1, keepdims=True)
    normed = (centred * lax.rsqrt(variance + 1e-05) * gain_ref[...]).astype(BF16)
    normed_ref[...] = normed
    outgoing_ref[...] = dot(of_block(pick_ref, send_ref).astype(BF16), normed).astype(BF16)


def mlp(token_rows, weight_in, weight_out):
    activation = jax.nn.gelu(dot(token_rows, weight_in), approximate=True).astype(BF16)
    return dot(activation, weight_out)


def layer_kernel(
    pick_ref,
    received_ref,
    normed_ref,
    incoming_ref,
    picked_ref,
    router_ref,
    dense_in_ref,
    dense_out_ref,
    expert_in_ref,
    expert_out_ref,
    result_ref,
    base_ref,
    gate_ref,
):
    sources, rows, model_width = incoming_ref.shape
    half = rows // 2
    late = (lax.axis_index("section") >= lax.axis_size("section") // 2).astype(jnp.int32)
    normed = normed_ref[...]
    logits = dot_t(normed, router_ref[...])
    picked = of_block(pick_ref, picked_ref)[:, : logits.shape[1]]
    logit = jnp.sum(picked * logits, axis=1, keepdims=True)
    gate_ref[...] = jnp.broadcast_to(jax.nn.sigmoid(logit), gate_ref.shape)
    dense_part = mlp(normed, dense_in_ref[...], dense_out_ref[...])
    base_ref[...] = received_ref[...].astype(F32) + dense_part
    for which, held in ((0, 0), (1, late)):
        window = pl.ds(which * half, half)
        token_rows = incoming_ref[:, window, :].reshape(sources * half, model_width)
        found = mlp(token_rows, expert_in_ref[held], expert_out_ref[held]).astype(BF16)
        result_ref[:, window, :] = found.reshape(sources, half, model_width)


def stream_after(pick_ref, base_ref, gate_ref, send_ref, returned_ref):
    routed = dot(of_block(pick_ref, send_ref).T.astype(BF16), returned_ref[...])
    return (base_ref[...] + gate_ref[:, :1] * routed).astype(BF16)


def leave_kernel(pick_ref, base_ref, gate_ref, send_ref, returned_ref, stream_ref):
    stream_ref[...] = stream_after(pick_ref, base_ref, gate_ref, send_ref, returned_ref)


def put_shares(stream, out_ref):
    share = out_ref.shape[2]
    for number in range(out_ref.shape[0]):
        out_ref[number] = stream[:, number * share : (number + 1) * share]


def finish_kernel(pick_ref, base_ref, gate_ref, send_ref, returned_ref, out_ref):
    put_shares(stream_after(pick_ref, base_ref, gate_ref, send_ref, returned_ref), out_ref)


def split_kernel(stream_ref, out_ref):
    put_shares(stream_ref[...], out_ref)


def gather_kernel(pieces_ref, out_ref):
    last = pieces_ref.shape[0] - 1
    out_ref[0] = pieces_ref[last - 1]
    out_ref[1] = pieces_ref[last]


def untouched_kernel(*refs):
    pass


def wait_kernel(turns, source_ref, target_ref, sems):
    groups = 8
    rows = source_ref.shape[0] // groups

    def turn(number, _):
        window = pl.ds(pl.multiple_of(number % groups * rows, rows), rows)
        copy = pltpu.make_async_copy(source_ref.at[window], target_ref.at[window], sems.at[0])
        copy.start()
        copy.wait()
        return 0

    lax.fori_loop(0, turns, turn, 0)


def copy_over_kernel(*refs):
    count = (len(refs) - 1) // 3
    sources, targets, stages, sems = refs[: count + 1], refs[count + 1 : 2 * count + 2], refs[2 * count + 2 : -1], refs[-1]

    @pl.when(lax.axis_index("section") >= 2)
    def _():
        reads = [
            pltpu.make_async_copy(source, stage, sems.at[0, n])
            for n, (source, stage) in enumerate(zip(sources, stages + targets[-1:]))
        ]
        writes = [
            pltpu.make_async_copy(stage, target, sems.at[1, n])
            for n, (stage, target) in enumerate(zip(stages, targets))
        ]
        for read in reads:
            read.start()
        for read, write in zip(reads, writes):
            read.wait()
            write.start()
        reads[-1].wait()
        for write in writes:
            write.wait()


def in_hbm(value):
    return pltpu.with_memory_space_constraint(value, pltpu.HBM)


def keep_kernel(source_ref, target_ref):
    target_ref[...] = source_ref[...]


def shape(dims, dtype):
    return jax.ShapeDtypeStruct(dims, dtype)


def kernel_call(kernel, inputs, outputs, cost=None):
    several = isinstance(outputs, tuple)
    return pl.pallas_call(
        kernel,
        out_shape=outputs,
        in_specs=[VMEM_SPEC] * inputs,
        out_specs=[VMEM_SPEC] * len(outputs) if several else VMEM_SPEC,
        cost_estimate=cost,
        compiler_params=pltpu.CompilerParams(vmem_limit_bytes=LIMIT),
    )


def body(tokens_in, ln_gain, router, dense_in, dense_out, expert_in, expert_out, routes):
    sections = lax.axis_size("section")
    members = lax.axis_size("expert")
    section_index = lax.axis_index("section")
    blocks, tok_dev, model_width = tokens_in.shape
    labels = router.shape[2]
    hidden_width = dense_in.shape[2]
    capacity = 2 * (tok_dev // labels)
    slots = labels * capacity
    share = model_width // sections
    stream_shape = shape((tok_dev, model_width), BF16)
    table_shapes = (
        shape((blocks, slots, tok_dev), BF16),
        shape((blocks, tok_dev, 128), F32),
        shape(ln_gain.shape, F32),
    )
    odd = section_index % 2
    own_block = odd

    def tables(always, ids, gain, *tokens):
        outputs = table_shapes + (stream_shape,) * (2 * len(tokens))
        return pl.pallas_call(
            functools.partial(tables_kernel, blocks, always),
            out_shape=outputs,
            in_specs=[pl.BlockSpec(memory_space=pltpu.HBM)] * (2 + len(tokens)),
            out_specs=[VMEM_SPEC] * len(outputs),
            scratch_shapes=[
                pltpu.VMEM((blocks, tok_dev), jnp.int32),
                pltpu.SemaphoreType.DMA((4,)),
            ],
            compiler_params=pltpu.CompilerParams(vmem_limit_bytes=LIMIT),
        )(*map(in_hbm, (ids, gain) + tokens))

    def pick(block):
        return jnp.full((8, 128), block, jnp.int32)

    def exchange(rows, axis):
        return lax.all_to_all(rows, axis, split_axis=0, concat_axis=0, tiled=True)

    ids = routes.reshape(blocks, tok_dev)
    router_rows = router[0].T
    weights = (dense_in[0], dense_out[0], expert_in[0], expert_out[0])
    *own_tables, first, second = tables(True, ids, ln_gain, tokens_in)
    own = (tuple(own_tables), router_rows, weights)

    def swapped():
        swap = [(source, source + 1 - 2 * (source % 2)) for source in range(sections)]
        arrays = weights + (router_rows, ids, ln_gain)
        return tuple(lax.ppermute(value, "section", swap) for value in arrays)

    def nothing():
        arrays = weights + (router_rows, ids, ln_gain)
        return tuple(
            pl.pallas_call(
                untouched_kernel,
                out_shape=tuple(shape(value.shape, value.dtype) for value in arrays),
                out_specs=[pl.BlockSpec(memory_space=pl.ANY)] * len(arrays),
            )()
        )

    *others, other_ids, other_gain = lax.cond(section_index >= 2, swapped, nothing)
    *other_weights, other_router = pl.pallas_call(
        copy_over_kernel,
        out_shape=tuple(shape(value.shape, value.dtype) for value in others),
        in_specs=[pl.BlockSpec(memory_space=pl.ANY)] * 5,
        out_specs=[pl.BlockSpec(memory_space=pl.ANY)] * 4 + [VMEM_SPEC],
        scratch_shapes=[pltpu.VMEM(value.shape, BF16) for value in weights]
        + [pltpu.SemaphoreType.DMA((2, 5))],
        compiler_params=pltpu.CompilerParams(vmem_limit_bytes=LIMIT),
    )(*others)
    other = (tuple(tables(False, other_ids, other_gain)), other_router, tuple(other_weights))

    def layer(block, received, context):
        (send, picked, gain), router_part, layer_weights = context
        chosen = pick(block)
        normed, outgoing = kernel_call(
            enter_kernel,
            4,
            (stream_shape, shape((slots, model_width), BF16)),
            pl.CostEstimate(flops=20_000_000_000, transcendentals=0, bytes_accessed=40 << 20),
        )(chosen, received, gain, send)
        incoming = exchange(outgoing.reshape(members, slots // members, model_width), "expert")
        results, base, gate = kernel_call(
            layer_kernel,
            10,
            (
                shape(incoming.shape, BF16),
                shape((tok_dev, model_width), F32),
                shape((tok_dev, 128), F32),
            ),
            pl.CostEstimate(
                flops=12 * tok_dev * model_width * hidden_width,
                transcendentals=3 * tok_dev * hidden_width,
                bytes_accessed=26 << 20,
            ),
        )(chosen, received, normed, incoming, picked, router_part, *layer_weights)
        returned = exchange(results, "expert").reshape(slots, model_width)
        return chosen, base, gate, send, returned

    def run(block, received, context):
        return kernel_call(leave_kernel, 5, stream_shape)(
            *layer(block, received, context)
        )

    def keep(stream):
        return kernel_call(keep_kernel, 1, stream_shape)(stream)

    def late_start(stream):
        return pl.pallas_call(
            functools.partial(wait_kernel, TURNS),
            out_shape=stream_shape,
            in_specs=[VMEM_SPEC],
            out_specs=VMEM_SPEC,
            scratch_shapes=[pltpu.SemaphoreType.DMA((1,))],
        )(stream)

    everyone = [(source, source) for source in range(sections)]
    pair = [(0, 1), (1, 0)] + everyone[2:]
    around = [(source, (source + 1) % sections) for source in range(sections)]
    odd_ring = everyone[0::2] + [(source, (source + 2) % sections) for source in range(1, sections, 2)]
    even_ring = everyone[1::2] + [(source, (source + 2) % sections) for source in range(0, sections, 2)]

    fresh = lax.cond(
        section_index == 0,
        lambda stream: run(0, stream, own),
        lambda stream: jnp.zeros((tok_dev, model_width), BF16),
        first,
    )
    arrived = lax.ppermute(fresh, "section", pair)
    waiting = lax.cond(
        section_index == 0,
        lambda stream: run(1, stream, own),
        lambda stream: jnp.zeros((tok_dev, model_width), BF16),
        second,
    )
    stream = lax.cond(
        section_index == 1,
        lambda arrived, waiting: run(0, late_start(arrived), own),
        lambda arrived, waiting: keep(waiting),
        arrived,
        waiting,
    )
    stream = keep(lax.ppermute(stream, "section", around))

    def chip(number, stream):
        place = section_index - 2 * number
        stream = lax.cond(
            (place == -1) | (place == 0),
            lambda stream: run(own_block, stream, own),
            keep,
            stream,
        )
        stream = lax.cond(
            odd == 1, lambda stream: keep(lax.ppermute(stream, "section", odd_ring)), keep, stream
        )
        stream = lax.cond(
            (place == 0) | (place == 1),
            lambda stream: run(own_block, stream, other),
            keep,
            stream,
        )
        return lax.cond(
            (odd == 0) & (number < sections // 2 - 1),
            lambda stream: keep(lax.ppermute(stream, "section", even_ring)),
            keep,
            stream,
        )

    stream = lax.fori_loop(1, sections // 2, chip, stream)
    pieces_shape = shape((sections, tok_dev, share), BF16)
    pieces = lax.cond(
        section_index == sections - 1,
        lambda stream: kernel_call(finish_kernel, 5, pieces_shape)(*layer(1, stream, own)),
        lambda stream: kernel_call(split_kernel, 1, pieces_shape)(stream),
        stream,
    )
    return kernel_call(gather_kernel, 1, shape((blocks, tok_dev, share), BF16))(
        exchange(pieces, "section")
    )


def solution(mesh):
    placed = (
        P(None, "expert", None),
        P("section", None),
        P("section", None, None),
        P("section", None, None),
        P("section", None, None),
        P("section", "expert", None, None),
        P("section", "expert", None, None),
        P("section", None, "expert", None),
    )
    return jax.shard_map(
        body, mesh=mesh, in_specs=placed, out_specs=P(None, "expert", "section"), check_vma=False
    )
```

```python
import functools

import jax
import jax.numpy as jnp
from jax import lax
from jax.experimental import pallas as pl
from jax.experimental.pallas import tpu as pltpu
from jax.sharding import PartitionSpec as P

BF16 = jnp.bfloat16
F32 = jnp.float32
VMEM_SPEC = pl.BlockSpec(memory_space=pltpu.VMEM)
LIMIT = 30 << 20
TURNS = 22


def dot(a, b):
    return jnp.dot(a, b, preferred_element_type=F32)


def dot_t(a, b):
    return lax.dot_general(a, b, (((1,), (1,)), ((), ())), preferred_element_type=F32)


def make_tables(blocks, routes_ref, gain_ref, *refs):
    tokens_ref = refs[0] if len(refs) == 8 else None
    send_ref, picked_ref, held_gain_ref = refs[1:4] if tokens_ref is not None else refs[:3]
    ids_ref, sems = refs[-2:]
    tokens = ids_ref.shape[1]
    moves = [(routes_ref, ids_ref), (gain_ref, held_gain_ref)]
    if tokens_ref is not None:
        moves += [(tokens_ref.at[0], refs[4]), (tokens_ref.at[1], refs[5])]
    copies = [
        pltpu.make_async_copy(source, target, sems.at[number])
        for number, (source, target) in enumerate(moves)
    ]
    for copy in copies:
        copy.start()
    copies[0].wait()
    slots = send_ref.shape[1]
    labels = picked_ref.shape[2]
    earlier = (
        lax.broadcasted_iota(jnp.int32, (tokens, tokens), 0)
        < lax.broadcasted_iota(jnp.int32, (tokens, tokens), 1)
    ).astype(BF16)
    capacity = slots // (labels // 4)
    for block in range(blocks):
        ids = ids_ref[block : block + 1, :]
        picked = (lax.broadcasted_iota(jnp.int32, (labels, tokens), 0) == ids).astype(F32)
        before = dot(picked.astype(BF16), earlier)
        position = jnp.sum(before * picked, axis=0, keepdims=True).astype(jnp.int32)
        slot = ids * capacity + position
        send = (lax.broadcasted_iota(jnp.int32, (slots, tokens), 0) == slot).astype(F32)
        send_ref[block] = send.astype(BF16)
        picked_ref[block] = picked.T
    for copy in copies[1:]:
        copy.wait()


def tables_kernel(blocks, always, *refs):
    if always:
        make_tables(blocks, *refs)
    else:
        pl.when(lax.axis_index("section") >= 2)(functools.partial(make_tables, blocks, *refs))


def of_block(pick_ref, table_ref):
    rows, lanes = table_ref.shape[1:]
    second = jnp.broadcast_to(pick_ref[:1, :1] == 1, (rows, lanes))
    return jnp.where(second, table_ref[1].astype(F32), table_ref[0].astype(F32))


def enter_kernel(
    pick_ref, received_ref, gain_ref, send_ref, normed_ref, outgoing_ref, stream_ref
):
    stream_ref[...] = received_ref[...]
    stream = received_ref[...].astype(F32)
    centred = stream - jnp.mean(stream, axis=-1, keepdims=True)
    variance = jnp.mean(centred * centred, axis=-1, keepdims=True)
    normed = (centred * lax.rsqrt(variance + 1e-05) * gain_ref[...]).astype(BF16)
    normed_ref[...] = normed
    outgoing_ref[...] = dot(of_block(pick_ref, send_ref).astype(BF16), normed).astype(BF16)


def mlp(token_rows, weight_in, weight_out):
    activation = jax.nn.gelu(dot(token_rows, weight_in), approximate=True).astype(BF16)
    return dot(activation, weight_out)


def layer_kernel(
    pick_ref,
    received_ref,
    normed_ref,
    incoming_ref,
    picked_ref,
    router_ref,
    dense_in_ref,
    dense_out_ref,
    expert_in_ref,
    expert_out_ref,
    result_ref,
    base_ref,
    gate_ref,
):
    sources, rows, model_width = incoming_ref.shape
    half = rows // 2
    late = (lax.axis_index("section") >= lax.axis_size("section") // 2).astype(jnp.int32)
    normed = normed_ref[...]
    logits = dot_t(normed, router_ref[...])
    picked = of_block(pick_ref, picked_ref)[:, : logits.shape[1]]
    logit = jnp.sum(picked * logits, axis=1, keepdims=True)
    gate_ref[...] = jnp.broadcast_to(jax.nn.sigmoid(logit), gate_ref.shape)
    dense_part = mlp(normed, dense_in_ref[...], dense_out_ref[...])
    base_ref[...] = received_ref[...].astype(F32) + dense_part
    for which, held in ((0, 0), (1, late)):
        window = pl.ds(which * half, half)
        token_rows = incoming_ref[:, window, :].reshape(sources * half, model_width)
        found = mlp(token_rows, expert_in_ref[held], expert_out_ref[held]).astype(BF16)
        result_ref[:, window, :] = found.reshape(sources, half, model_width)


def stream_after(pick_ref, base_ref, gate_ref, send_ref, returned_ref):
    routed = dot(of_block(pick_ref, send_ref).T.astype(BF16), returned_ref[...])
    return (base_ref[...] + gate_ref[:, :1] * routed).astype(BF16)


def leave_kernel(pick_ref, base_ref, gate_ref, send_ref, returned_ref, stream_ref):
    stream_ref[...] = stream_after(pick_ref, base_ref, gate_ref, send_ref, returned_ref)


def put_shares(stream, out_ref):
    share = out_ref.shape[2]
    for number in range(out_ref.shape[0]):
        out_ref[number] = stream[:, number * share : (number + 1) * share]


def finish_kernel(pick_ref, base_ref, gate_ref, send_ref, returned_ref, out_ref):
    put_shares(stream_after(pick_ref, base_ref, gate_ref, send_ref, returned_ref), out_ref)


def split_kernel(stream_ref, out_ref):
    put_shares(stream_ref[...], out_ref)


def gather_kernel(pieces_ref, out_ref):
    last = pieces_ref.shape[0] - 1
    out_ref[0] = pieces_ref[last - 1]
    out_ref[1] = pieces_ref[last]


def untouched_kernel(*refs):
    pass


def wait_kernel(turns, source_ref, target_ref, sems):
    groups = 8
    rows = source_ref.shape[0] // groups

    def turn(number, _):
        window = pl.ds(pl.multiple_of(number % groups * rows, rows), rows)
        copy = pltpu.make_async_copy(source_ref.at[window], target_ref.at[window], sems.at[0])
        copy.start()
        copy.wait()
        return 0

    lax.fori_loop(0, turns, turn, 0)


def copy_over_kernel(*refs):
    count = (len(refs) - 1) // 3
    sources, targets, stages, sems = refs[: count + 1], refs[count + 1 : 2 * count + 2], refs[2 * count + 2 : -1], refs[-1]

    @pl.when(lax.axis_index("section") >= 2)
    def _():
        reads = [
            pltpu.make_async_copy(source, stage, sems.at[0, n])
            for n, (source, stage) in enumerate(zip(sources, stages + targets[-1:]))
        ]
        writes = [
            pltpu.make_async_copy(stage, target, sems.at[1, n])
            for n, (stage, target) in enumerate(zip(stages, targets))
        ]
        for read in reads:
            read.start()
        for read, write in zip(reads, writes):
            read.wait()
            write.start()
        reads[-1].wait()
        for write in writes:
            write.wait()


def in_hbm(value):
    return pltpu.with_memory_space_constraint(value, pltpu.HBM)


def keep_kernel(source_ref, target_ref):
    target_ref[...] = source_ref[...]


def shape(dims, dtype):
    return jax.ShapeDtypeStruct(dims, dtype)


def kernel_call(kernel, inputs, outputs, cost=None):
    several = isinstance(outputs, tuple)
    return pl.pallas_call(
        kernel,
        out_shape=outputs,
        in_specs=[VMEM_SPEC] * inputs,
        out_specs=[VMEM_SPEC] * len(outputs) if several else VMEM_SPEC,
        cost_estimate=cost,
        compiler_params=pltpu.CompilerParams(vmem_limit_bytes=LIMIT),
    )


def body(tokens_in, ln_gain, router, dense_in, dense_out, expert_in, expert_out, routes):
    sections = lax.axis_size("section")
    members = lax.axis_size("expert")
    section_index = lax.axis_index("section")
    blocks, tok_dev, model_width = tokens_in.shape
    labels = router.shape[2]
    hidden_width = dense_in.shape[2]
    capacity = 2 * (tok_dev // labels)
    slots = labels * capacity
    share = model_width // sections
    stream_shape = shape((tok_dev, model_width), BF16)
    table_shapes = (
        shape((blocks, slots, tok_dev), BF16),
        shape((blocks, tok_dev, 128), F32),
        shape(ln_gain.shape, F32),
    )
    odd = section_index % 2
    own_block = odd

    def tables(always, ids, gain, *tokens):
        outputs = table_shapes + (stream_shape,) * (2 * len(tokens))
        return pl.pallas_call(
            functools.partial(tables_kernel, blocks, always),
            out_shape=outputs,
            in_specs=[pl.BlockSpec(memory_space=pltpu.HBM)] * (2 + len(tokens)),
            out_specs=[VMEM_SPEC] * len(outputs),
            scratch_shapes=[
                pltpu.VMEM((blocks, tok_dev), jnp.int32),
                pltpu.SemaphoreType.DMA((4,)),
            ],
            compiler_params=pltpu.CompilerParams(vmem_limit_bytes=LIMIT),
        )(*map(in_hbm, (ids, gain) + tokens))

    def pick(block):
        return jnp.full((8, 128), block, jnp.int32)

    def exchange(rows, axis):
        return lax.all_to_all(rows, axis, split_axis=0, concat_axis=0, tiled=True)

    ids = routes.reshape(blocks, tok_dev)
    router_rows = router[0].T
    weights = (dense_in[0], dense_out[0], expert_in[0], expert_out[0])
    *own_tables, first, second = tables(True, ids, ln_gain, tokens_in)
    own = (tuple(own_tables), router_rows, weights)

    def swapped():
        swap = [(source, source + 1 - 2 * (source % 2)) for source in range(sections)]
        arrays = weights + (router_rows, ids, ln_gain)
        return tuple(lax.ppermute(value, "section", swap) for value in arrays)

    def nothing():
        arrays = weights + (router_rows, ids, ln_gain)
        return tuple(
            pl.pallas_call(
                untouched_kernel,
                out_shape=tuple(shape(value.shape, value.dtype) for value in arrays),
                out_specs=[pl.BlockSpec(memory_space=pl.ANY)] * len(arrays),
            )()
        )

    *others, other_ids, other_gain = lax.cond(section_index >= 2, swapped, nothing)
    *other_weights, other_router = pl.pallas_call(
        copy_over_kernel,
        out_shape=tuple(shape(value.shape, value.dtype) for value in others),
        in_specs=[pl.BlockSpec(memory_space=pl.ANY)] * 5,
        out_specs=[pl.BlockSpec(memory_space=pl.ANY)] * 4 + [VMEM_SPEC],
        scratch_shapes=[pltpu.VMEM(value.shape, BF16) for value in weights]
        + [pltpu.SemaphoreType.DMA((2, 5))],
        compiler_params=pltpu.CompilerParams(vmem_limit_bytes=LIMIT),
    )(*others)
    other = (tuple(tables(False, other_ids, other_gain)), other_router, tuple(other_weights))

    def layer(block, received, context):
        (send, picked, gain), router_part, layer_weights = context
        chosen = pick(block)
        normed, outgoing, received = kernel_call(
            enter_kernel,
            4,
            (stream_shape, shape((slots, model_width), BF16), stream_shape),
            pl.CostEstimate(flops=20_000_000_000, transcendentals=0, bytes_accessed=40 << 20),
        )(chosen, received, gain, send)
        incoming = exchange(outgoing.reshape(members, slots // members, model_width), "expert")
        results, base, gate = kernel_call(
            layer_kernel,
            10,
            (
                shape(incoming.shape, BF16),
                shape((tok_dev, model_width), F32),
                shape((tok_dev, 128), F32),
            ),
            pl.CostEstimate(
                flops=12 * tok_dev * model_width * hidden_width,
                transcendentals=3 * tok_dev * hidden_width,
                bytes_accessed=26 << 20,
            ),
        )(chosen, received, normed, incoming, picked, router_part, *layer_weights)
        returned = exchange(results, "expert").reshape(slots, model_width)
        return chosen, base, gate, send, returned

    def run(block, received, context):
        return kernel_call(leave_kernel, 5, stream_shape)(
            *layer(block, received, context)
        )

    def keep(stream):
        return kernel_call(keep_kernel, 1, stream_shape)(stream)

    def late_start(stream):
        return pl.pallas_call(
            functools.partial(wait_kernel, TURNS),
            out_shape=stream_shape,
            in_specs=[VMEM_SPEC],
            out_specs=VMEM_SPEC,
            scratch_shapes=[pltpu.SemaphoreType.DMA((1,))],
        )(stream)

    around = [(source, (source + 1) % sections) for source in range(sections)]
    two_on = [(source, (source + 2) % sections) for source in range(sections)]

    fresh = lax.cond(
        section_index == 0,
        lambda stream: run(0, stream, own),
        lambda stream: jnp.zeros((tok_dev, model_width), BF16),
        first,
    )
    arrived = lax.ppermute(fresh, "section", around)
    waiting = lax.cond(
        section_index == 0,
        lambda stream: run(1, stream, own),
        lambda stream: jnp.zeros((tok_dev, model_width), BF16),
        second,
    )
    stream = lax.cond(
        section_index == 1,
        lambda arrived, waiting: run(0, late_start(arrived), own),
        lambda arrived, waiting: keep(waiting),
        arrived,
        waiting,
    )
    stream = lax.ppermute(stream, "section", around)

    def chip(number, stream):
        place = section_index - 2 * number
        stream = lax.switch(
            jnp.where(odd == 1, 0, jnp.where(number > 1, 1, 2)),
            (
                keep,
                lambda stream: keep(lax.ppermute(stream, "section", two_on)),
                late_start,
            ),
            stream,
        )
        stream = lax.cond(
            (place == -1) | (place == 0),
            lambda stream: run(own_block, stream, own),
            keep,
            stream,
        )
        stream = lax.cond(
            odd == 1, lambda stream: keep(lax.ppermute(stream, "section", two_on)), keep, stream
        )
        stream = lax.cond(
            (place == 0) | (place == 1),
            lambda stream: run(own_block, stream, other),
            keep,
            stream,
        )
        return stream

    stream = lax.fori_loop(1, sections // 2, chip, stream)
    pieces_shape = shape((sections, tok_dev, share), BF16)
    pieces = lax.cond(
        section_index == sections - 1,
        lambda stream: kernel_call(finish_kernel, 5, pieces_shape)(*layer(1, stream, own)),
        lambda stream: kernel_call(split_kernel, 1, pieces_shape)(stream),
        stream,
    )
    return kernel_call(gather_kernel, 1, shape((blocks, tok_dev, share), BF16))(
        exchange(pieces, "section")
    )


def solution(mesh):
    placed = (
        P(None, "expert", None),
        P("section", None),
        P("section", None, None),
        P("section", None, None),
        P("section", None, None),
        P("section", "expert", None, None),
        P("section", "expert", None, None),
        P("section", None, "expert", None),
    )
    return jax.shard_map(
        body, mesh=mesh, in_specs=placed, out_specs=P(None, "expert", "section"), check_vma=False
    )
```

```python
import functools

import jax
import jax.numpy as jnp
from jax import lax
from jax.experimental import pallas as pl
from jax.experimental.pallas import tpu as pltpu
from jax.sharding import PartitionSpec as P

BF16 = jnp.bfloat16
F32 = jnp.float32
VMEM_SPEC = pl.BlockSpec(memory_space=pltpu.VMEM)
LIMIT = 30 << 20
FIRST_TURNS = 22
SECOND_TURNS = 50


def dot(a, b):
    return jnp.dot(a, b, preferred_element_type=F32)


def dot_t(a, b):
    return lax.dot_general(a, b, (((1,), (1,)), ((), ())), preferred_element_type=F32)


def make_tables(blocks, routes_ref, gain_ref, *refs):
    tokens_ref = refs[0] if len(refs) == 8 else None
    send_ref, picked_ref, held_gain_ref = refs[1:4] if tokens_ref is not None else refs[:3]
    ids_ref, sems = refs[-2:]
    tokens = ids_ref.shape[1]
    moves = [(routes_ref, ids_ref), (gain_ref, held_gain_ref)]
    if tokens_ref is not None:
        moves += [(tokens_ref.at[0], refs[4]), (tokens_ref.at[1], refs[5])]
    copies = [
        pltpu.make_async_copy(source, target, sems.at[number])
        for number, (source, target) in enumerate(moves)
    ]
    for copy in copies:
        copy.start()
    copies[0].wait()
    slots = send_ref.shape[1]
    labels = picked_ref.shape[2]
    earlier = (
        lax.broadcasted_iota(jnp.int32, (tokens, tokens), 0)
        < lax.broadcasted_iota(jnp.int32, (tokens, tokens), 1)
    ).astype(BF16)
    capacity = slots // (labels // 4)
    for block in range(blocks):
        ids = ids_ref[block : block + 1, :]
        picked = (lax.broadcasted_iota(jnp.int32, (labels, tokens), 0) == ids).astype(F32)
        before = dot(picked.astype(BF16), earlier)
        position = jnp.sum(before * picked, axis=0, keepdims=True).astype(jnp.int32)
        slot = ids * capacity + position
        send = (lax.broadcasted_iota(jnp.int32, (slots, tokens), 0) == slot).astype(F32)
        send_ref[block] = send.astype(BF16)
        picked_ref[block] = picked.T
    for copy in copies[1:]:
        copy.wait()


def tables_kernel(blocks, always, *refs):
    if always:
        make_tables(blocks, *refs)
    else:
        pl.when(lax.axis_index("section") >= 2)(functools.partial(make_tables, blocks, *refs))


def of_block(pick_ref, table_ref):
    rows, lanes = table_ref.shape[1:]
    second = jnp.broadcast_to(pick_ref[:1, :1] == 1, (rows, lanes))
    return jnp.where(second, table_ref[1].astype(F32), table_ref[0].astype(F32))


def enter_kernel(
    pick_ref, received_ref, gain_ref, send_ref, normed_ref, outgoing_ref, stream_ref
):
    stream_ref[...] = received_ref[...]
    stream = received_ref[...].astype(F32)
    centred = stream - jnp.mean(stream, axis=-1, keepdims=True)
    variance = jnp.mean(centred * centred, axis=-1, keepdims=True)
    normed = (centred * lax.rsqrt(variance + 1e-05) * gain_ref[...]).astype(BF16)
    normed_ref[...] = normed
    outgoing_ref[...] = dot(of_block(pick_ref, send_ref).astype(BF16), normed).astype(BF16)


def mlp(token_rows, weight_in, weight_out):
    activation = jax.nn.gelu(dot(token_rows, weight_in), approximate=True).astype(BF16)
    return dot(activation, weight_out)


def layer_kernel(
    pick_ref,
    received_ref,
    normed_ref,
    incoming_ref,
    picked_ref,
    router_ref,
    dense_in_ref,
    dense_out_ref,
    expert_in_ref,
    expert_out_ref,
    result_ref,
    base_ref,
    gate_ref,
):
    sources, rows, model_width = incoming_ref.shape
    half = rows // 2
    late = (lax.axis_index("section") >= lax.axis_size("section") // 2).astype(jnp.int32)
    normed = normed_ref[...]
    logits = dot_t(normed, router_ref[...])
    picked = of_block(pick_ref, picked_ref)[:, : logits.shape[1]]
    logit = jnp.sum(picked * logits, axis=1, keepdims=True)
    gate_ref[...] = jnp.broadcast_to(jax.nn.sigmoid(logit), gate_ref.shape)
    dense_part = mlp(normed, dense_in_ref[...], dense_out_ref[...])
    base_ref[...] = received_ref[...].astype(F32) + dense_part
    for which, held in ((0, 0), (1, late)):
        window = pl.ds(which * half, half)
        token_rows = incoming_ref[:, window, :].reshape(sources * half, model_width)
        found = mlp(token_rows, expert_in_ref[held], expert_out_ref[held]).astype(BF16)
        result_ref[:, window, :] = found.reshape(sources, half, model_width)


def stream_after(pick_ref, base_ref, gate_ref, send_ref, returned_ref):
    routed = dot(of_block(pick_ref, send_ref).T.astype(BF16), returned_ref[...])
    return (base_ref[...] + gate_ref[:, :1] * routed).astype(BF16)


def leave_kernel(pick_ref, base_ref, gate_ref, send_ref, returned_ref, stream_ref):
    stream_ref[...] = stream_after(pick_ref, base_ref, gate_ref, send_ref, returned_ref)


def put_shares(stream, out_ref):
    share = out_ref.shape[2]
    for number in range(out_ref.shape[0]):
        out_ref[number] = stream[:, number * share : (number + 1) * share]


def finish_kernel(pick_ref, base_ref, gate_ref, send_ref, returned_ref, out_ref):
    put_shares(stream_after(pick_ref, base_ref, gate_ref, send_ref, returned_ref), out_ref)


def split_kernel(stream_ref, out_ref):
    put_shares(stream_ref[...], out_ref)


def gather_kernel(pieces_ref, out_ref):
    last = pieces_ref.shape[0] - 1
    out_ref[0] = pieces_ref[last - 1]
    out_ref[1] = pieces_ref[last]


def untouched_kernel(*refs):
    pass


def wait_kernel(turns, source_ref, target_ref, sems):
    groups = 8
    rows = source_ref.shape[0] // groups

    def turn(number, _):
        window = pl.ds(pl.multiple_of(number % groups * rows, rows), rows)
        copy = pltpu.make_async_copy(source_ref.at[window], target_ref.at[window], sems.at[0])
        copy.start()
        copy.wait()
        return 0

    lax.fori_loop(0, turns, turn, 0)


def copy_over_kernel(*refs):
    count = (len(refs) - 1) // 3
    sources, targets, stages, sems = refs[: count + 1], refs[count + 1 : 2 * count + 2], refs[2 * count + 2 : -1], refs[-1]

    @pl.when(lax.axis_index("section") >= 2)
    def _():
        reads = [
            pltpu.make_async_copy(source, stage, sems.at[0, n])
            for n, (source, stage) in enumerate(zip(sources, stages + targets[-1:]))
        ]
        writes = [
            pltpu.make_async_copy(stage, target, sems.at[1, n])
            for n, (stage, target) in enumerate(zip(stages, targets))
        ]
        for read in reads:
            read.start()
        for read, write in zip(reads, writes):
            read.wait()
            write.start()
        reads[-1].wait()
        for write in writes:
            write.wait()


def in_hbm(value):
    return pltpu.with_memory_space_constraint(value, pltpu.HBM)


def keep_kernel(source_ref, target_ref):
    target_ref[...] = source_ref[...]


def shape(dims, dtype):
    return jax.ShapeDtypeStruct(dims, dtype)


def kernel_call(kernel, inputs, outputs, cost=None):
    several = isinstance(outputs, tuple)
    return pl.pallas_call(
        kernel,
        out_shape=outputs,
        in_specs=[VMEM_SPEC] * inputs,
        out_specs=[VMEM_SPEC] * len(outputs) if several else VMEM_SPEC,
        cost_estimate=cost,
        compiler_params=pltpu.CompilerParams(vmem_limit_bytes=LIMIT),
    )


def body(tokens_in, ln_gain, router, dense_in, dense_out, expert_in, expert_out, routes):
    sections = lax.axis_size("section")
    members = lax.axis_size("expert")
    section_index = lax.axis_index("section")
    blocks, tok_dev, model_width = tokens_in.shape
    labels = router.shape[2]
    hidden_width = dense_in.shape[2]
    capacity = 2 * (tok_dev // labels)
    slots = labels * capacity
    share = model_width // sections
    stream_shape = shape((tok_dev, model_width), BF16)
    table_shapes = (
        shape((blocks, slots, tok_dev), BF16),
        shape((blocks, tok_dev, 128), F32),
        shape(ln_gain.shape, F32),
    )
    odd = section_index % 2
    own_block = odd

    def tables(always, ids, gain, *tokens):
        outputs = table_shapes + (stream_shape,) * (2 * len(tokens))
        return pl.pallas_call(
            functools.partial(tables_kernel, blocks, always),
            out_shape=outputs,
            in_specs=[pl.BlockSpec(memory_space=pltpu.HBM)] * (2 + len(tokens)),
            out_specs=[VMEM_SPEC] * len(outputs),
            scratch_shapes=[
                pltpu.VMEM((blocks, tok_dev), jnp.int32),
                pltpu.SemaphoreType.DMA((4,)),
            ],
            compiler_params=pltpu.CompilerParams(vmem_limit_bytes=LIMIT),
        )(*map(in_hbm, (ids, gain) + tokens))

    def pick(block):
        return jnp.full((8, 128), block, jnp.int32)

    def exchange(rows, axis):
        return lax.all_to_all(rows, axis, split_axis=0, concat_axis=0, tiled=True)

    ids = routes.reshape(blocks, tok_dev)
    router_rows = router[0].T
    weights = (dense_in[0], dense_out[0], expert_in[0], expert_out[0])
    *own_tables, first, second = tables(True, ids, ln_gain, tokens_in)
    own = (tuple(own_tables), router_rows, weights)

    def swapped():
        swap = [(source, source + 1 - 2 * (source % 2)) for source in range(sections)]
        arrays = weights + (router_rows, ids, ln_gain)
        return tuple(lax.ppermute(value, "section", swap) for value in arrays)

    def nothing():
        arrays = weights + (router_rows, ids, ln_gain)
        return tuple(
            pl.pallas_call(
                untouched_kernel,
                out_shape=tuple(shape(value.shape, value.dtype) for value in arrays),
                out_specs=[pl.BlockSpec(memory_space=pl.ANY)] * len(arrays),
            )()
        )

    *others, other_ids, other_gain = lax.cond(section_index >= 2, swapped, nothing)
    *other_weights, other_router = pl.pallas_call(
        copy_over_kernel,
        out_shape=tuple(shape(value.shape, value.dtype) for value in others),
        in_specs=[pl.BlockSpec(memory_space=pl.ANY)] * 5,
        out_specs=[pl.BlockSpec(memory_space=pl.ANY)] * 4 + [VMEM_SPEC],
        scratch_shapes=[pltpu.VMEM(value.shape, BF16) for value in weights]
        + [pltpu.SemaphoreType.DMA((2, 5))],
        compiler_params=pltpu.CompilerParams(vmem_limit_bytes=LIMIT),
    )(*others)
    other = (tuple(tables(False, other_ids, other_gain)), other_router, tuple(other_weights))

    def layer(block, received, context):
        (send, picked, gain), router_part, layer_weights = context
        chosen = pick(block)
        normed, outgoing, received = kernel_call(
            enter_kernel,
            4,
            (stream_shape, shape((slots, model_width), BF16), stream_shape),
            pl.CostEstimate(flops=20_000_000_000, transcendentals=0, bytes_accessed=40 << 20),
        )(chosen, received, gain, send)
        incoming = exchange(outgoing.reshape(members, slots // members, model_width), "expert")
        results, base, gate = kernel_call(
            layer_kernel,
            10,
            (
                shape(incoming.shape, BF16),
                shape((tok_dev, model_width), F32),
                shape((tok_dev, 128), F32),
            ),
            pl.CostEstimate(
                flops=12 * tok_dev * model_width * hidden_width,
                transcendentals=3 * tok_dev * hidden_width,
                bytes_accessed=26 << 20,
            ),
        )(chosen, received, normed, incoming, picked, router_part, *layer_weights)
        returned = exchange(results, "expert").reshape(slots, model_width)
        return chosen, base, gate, send, returned

    def run(block, received, context):
        return kernel_call(leave_kernel, 5, stream_shape)(
            *layer(block, received, context)
        )

    def keep(stream):
        return kernel_call(keep_kernel, 1, stream_shape)(stream)

    def late_start(turns, stream):
        return pl.pallas_call(
            functools.partial(wait_kernel, turns),
            out_shape=stream_shape,
            in_specs=[VMEM_SPEC],
            out_specs=VMEM_SPEC,
            scratch_shapes=[pltpu.SemaphoreType.DMA((1,))],
        )(stream)

    around = [(source, (source + 1) % sections) for source in range(sections)]
    first_pair = [(0, 1), (1, 0)] + [(source, source) for source in range(2, sections)]
    two_on = [(source, (source + 2) % sections) for source in range(sections)]

    fresh = lax.cond(
        section_index == 0,
        lambda stream: run(0, stream, own),
        lambda stream: jnp.zeros((tok_dev, model_width), BF16),
        first,
    )
    arrived = lax.ppermute(fresh, "section", first_pair)
    waiting = lax.cond(
        section_index == 0,
        lambda stream: run(1, stream, own),
        lambda stream: jnp.zeros((tok_dev, model_width), BF16),
        second,
    )
    stream = lax.cond(
        section_index == 1,
        lambda arrived, waiting: run(0, late_start(FIRST_TURNS, arrived), own),
        lambda arrived, waiting: keep(waiting),
        arrived,
        waiting,
    )
    stream = lax.ppermute(stream, "section", around)

    def chip(number, stream):
        place = section_index - 2 * number
        stream = lax.switch(
            jnp.where(odd == 1, 0, jnp.where(number > 1, 1, 2)),
            (
                keep,
                lambda stream: keep(lax.ppermute(stream, "section", two_on)),
                functools.partial(late_start, SECOND_TURNS),
            ),
            stream,
        )
        stream = lax.cond(
            (place == -1) | (place == 0),
            lambda stream: run(own_block, stream, own),
            keep,
            stream,
        )
        stream = lax.cond(
            odd == 1, lambda stream: keep(lax.ppermute(stream, "section", two_on)), keep, stream
        )
        stream = lax.cond(
            (place == 0) | (place == 1),
            lambda stream: run(own_block, stream, other),
            keep,
            stream,
        )
        return stream

    stream = lax.fori_loop(1, sections // 2, chip, stream)
    pieces_shape = shape((sections, tok_dev, share), BF16)
    pieces = lax.cond(
        section_index == sections - 1,
        lambda stream: kernel_call(finish_kernel, 5, pieces_shape)(*layer(1, stream, own)),
        lambda stream: kernel_call(split_kernel, 1, pieces_shape)(stream),
        stream,
    )
    return kernel_call(gather_kernel, 1, shape((blocks, tok_dev, share), BF16))(
        exchange(pieces, "section")
    )


def solution(mesh):
    placed = (
        P(None, "expert", None),
        P("section", None),
        P("section", None, None),
        P("section", None, None),
        P("section", None, None),
        P("section", "expert", None, None),
        P("section", "expert", None, None),
        P("section", None, "expert", None),
    )
    return jax.shard_map(
        body, mesh=mesh, in_specs=placed, out_specs=P(None, "expert", "section"), check_vma=False
    )
```
